32 devices in a mesh: grp: 4 (over y, x), mem: 8 (over z, core).
Axes of the slice: x: 2, y: 2, z: 4, core: 2. Of those that a mesh axis runs over, the one named last changes fastest.
Arguments:
- values: bfloat16 [32, 8, 32, 128], P(('grp', 'mem')), may hold values from -6 to 6
- slots: int32 [32, 8, 32], P(('grp', 'mem')), may hold values from 0 to 7167
- counts: int32 [32, 8], P(('grp', 'mem')), may hold values from 0 to 32, as said below
Outputs:
- averaged: float32 [57344, 128], P('mem')
- returned: bfloat16 [32, 8, 32, 128], P(('grp', 'mem'))
The draws below stay inside these ranges and needn't reach their ends.
Inputs may be any that keep to these rules, and one draw needn't show every extreme that they name: `counts`: every device has at least one list with exactly 32 valid entries.
All inputs are finite; a program needn't handle non-finite values.
Results may differ from the reference program's by a relative error of at most 0.0024.
Values may be sent and summed in bfloat16 or wider, within the bound.
No kernel may reach another device: no remote copies, remote signals or barrier semaphores. Data moves between devices by JAX's collectives and lax.ppermute only.
A program may use at most 64 MiB of HBM per device.

```python
import jax
import jax.numpy as jnp

BLOCK = 128
BUCKET = 7168
CAP = 32
SENDERS = 32
N_MEM = 8


def draw_counts(key, part):
    key_load, key_base, key_full = jax.random.split(jax.random.fold_in(key, 7), 3)
    owner_load = jax.random.randint(key_load, (1, N_MEM), 1, 5)
    base_count = jax.random.randint(key_base, (SENDERS, N_MEM), 0, CAP + 1)
    scaled = jnp.minimum(base_count * owner_load // 2, CAP)
    full_list = jax.random.randint(key_full, (SENDERS, 1), 0, N_MEM)
    columns = jnp.arange(N_MEM, dtype=jnp.int32)[None, :]
    return jnp.where(columns == full_list, CAP, scaled).astype(jnp.int32)


def touch_ends(result, own_key, smallest, top_value):
    longest = result.shape.index(max(result.shape))
    spots = []
    for shift in (0, 1):
        where = [jax.random.randint(jax.random.fold_in(own_key, axis), (), 0, length) for axis, length in enumerate(result.shape)]
        where[longest] = (where[longest] + shift) % result.shape[longest]
        spots.append(tuple(where))
    return result.at[spots[0]].set(smallest).at[spots[1]].set(top_value)


def level_of(own_key, dims, cuts, low, high):
    def one(dim, parts):
        draws = jax.random.uniform(jax.random.fold_in(jax.random.fold_in(own_key, 6), dim), (parts,), jnp.float32, low / len(cuts), high / len(cuts))
        return jnp.repeat(jnp.exp(draws), dims[dim] // parts).reshape((-1,) + (1,) * (len(dims) - dim - 1))

    factor_of = one(*cuts[0])
    for cut in cuts[1:]:
        factor_of = factor_of * one(*cut)
    return factor_of


def noise(own_key, shape, deviation, limit, cuts=(), kind=jnp.bfloat16):
    drawn = deviation * jax.random.normal(own_key, shape, jnp.float32)
    if cuts:
        drawn = drawn * level_of(own_key, shape, cuts, -0.22, 0.18)
    return jnp.clip(drawn, -limit, limit).astype(kind)


def setup_inputs(seed: int = 0) -> dict:
    key_list = jax.random.split(jax.random.key(seed), 4)
    return {
        "values": noise(key_list[0], (SENDERS, N_MEM, CAP, BLOCK), 1.0, 6.0, ((0, 32),)),
        "slots": touch_ends(jax.random.randint(key_list[1], (SENDERS, N_MEM, CAP), 0, BUCKET), jax.random.fold_in(key_list[1], 1), 0, BUCKET - 1).astype(jnp.int32),
        "counts": draw_counts(jax.random.fold_in(key_list[3], 71), 0),
    }


def reference(values, slots, counts):
    is_valid = jnp.arange(CAP, dtype=jnp.int32)[None, None, :] < counts[:, :, None]
    target = (jnp.arange(N_MEM, dtype=jnp.int32)[None, :, None] * BUCKET + slots).reshape(-1)
    masked = jnp.where(is_valid[..., None], values.astype(jnp.float32), jnp.float32(0.0)).reshape(-1, BLOCK)
    slot_sums = jax.ops.segment_sum(masked, target, num_segments=N_MEM * BUCKET)
    slot_count = jax.ops.segment_sum(is_valid.reshape(-1).astype(jnp.float32), target, num_segments=N_MEM * BUCKET)
    averaged = slot_sums / jnp.maximum(slot_count, jnp.float32(1.0))[:, None]
    picked = jnp.take(averaged, target, axis=0).reshape(values.shape)
    returned = jnp.where(is_valid[..., None], picked, jnp.float32(0.0)).astype(jnp.bfloat16)
    return averaged, returned
```

```python
import functools
import math

import jax
import jax.numpy as jnp
from jax import lax
from jax.experimental import pallas as pl
from jax.experimental.pallas import tpu as pltpu
from jax.sharding import PartitionSpec as P

BUCKET = 7168
LANES = 128
META = 8


def vmem_spec():
    return pl.BlockSpec(memory_space=pltpu.VMEM)


def pack_kernel(groups, values_ref, slots_ref, counts_ref, out_ref):
    members, capacity, lanes = values_ref.shape
    shape = (members, members)
    diagonal = lax.broadcasted_iota(jnp.int32, shape, 0) == lax.broadcasted_iota(jnp.int32, shape, 1)
    count = jnp.sum(jnp.where(diagonal, counts_ref[...].astype(jnp.float32), 0.0), axis=1, keepdims=True)
    slot = slots_ref[...]
    place = lax.broadcasted_iota(jnp.int32, slot.shape, 1).astype(jnp.float32)
    live = place < count
    high = jnp.where(live, (slot // LANES).astype(jnp.float32), -1.0)
    low = jnp.where(live, (slot % LANES).astype(jnp.float32), 0.0)
    repeats = lanes // capacity
    high = jnp.concatenate([high] * repeats, axis=1)
    low = jnp.concatenate([low] * repeats, axis=1)
    row = lax.broadcasted_iota(jnp.int32, (members, META, lanes), 1)
    meta = jnp.where(row == 0, high[:, None, :], jnp.where(row == 1, low[:, None, :], 0.0))
    meta = meta.astype(jnp.bfloat16)
    for group in range(groups):
        rows = pl.ds(group * members, members)
        out_ref[rows, pl.ds(0, capacity), :] = values_ref[...]
        out_ref[rows, pl.ds(capacity, META), :] = meta


def pack(values, slots, counts, groups):
    members, capacity, lanes = values.shape
    return pl.pallas_call(
        functools.partial(pack_kernel, groups),
        out_shape=jax.ShapeDtypeStruct((groups * members, capacity + META, lanes), jnp.bfloat16),
        in_specs=[vmem_spec()] * 3,
        out_specs=vmem_spec(),
        name="pack",
    )(values, slots, counts)


def slots_of(lists_ref, first, senders, capacity):
    meta = lists_ref[pl.ds(first, senders), pl.ds(capacity, META), :].astype(jnp.float32)
    return meta[:, 0, :] * LANES + meta[:, 1, :]


def load_entries(lists_ref, rhs_ref, key_ref):
    senders, rows, lanes = lists_ref.shape
    capacity = rows - META
    slot = slots_of(lists_ref, 0, senders, capacity)
    per_block = lanes // capacity
    part = lax.broadcasted_iota(jnp.int32, (1, lanes), 1) // capacity
    for block in range(senders // per_block):
        key = slot[block * per_block : block * per_block + 1]
        for k in range(1, per_block):
            at = block * per_block + k
            key = jnp.where(part == k, slot[at : at + 1], key)
        key_ref[:, block * lanes : (block + 1) * lanes] = key
    rhs_ref[:, :lanes] = lists_ref[:, pl.ds(0, capacity), :].reshape(senders * capacity, lanes)
    rhs_ref[:, lanes:] = jnp.ones((senders * capacity, lanes), jnp.bfloat16)


def average(wanted, key_ref, rhs_ref):
    lanes = rhs_ref.shape[1] // 2
    onehot = (wanted == key_ref[...]).astype(jnp.float32).astype(jnp.bfloat16)
    both = jnp.dot(onehot, rhs_ref[...], preferred_element_type=jnp.float32)
    return both[:, :lanes] / jnp.maximum(both[:, lanes:], 1.0)


def answer_kernel(axis, step, lists_ref, out_ref, rhs_ref, key_ref):
    senders, rows, lanes = lists_ref.shape
    capacity = rows - META

    @pl.when(pl.program_id(0) == 0)
    def _():
        load_entries(lists_ref, rhs_ref, key_ref)

    members = step * pl.num_programs(0)
    first = lax.axis_index(axis) * members + pl.program_id(0) * step
    slot = slots_of(lists_ref, first, step, capacity)
    shape = (step, capacity, lanes)
    here = lax.broadcasted_iota(jnp.int32, shape, 2) == lax.broadcasted_iota(jnp.int32, shape, 1)
    column = jnp.sum(jnp.where(here, slot[:, None, :], 0.0), axis=2, keepdims=True)
    column = jnp.where(column < 0.0, -1.0, column).reshape(step * capacity, 1)
    out_ref[...] = average(column, key_ref, rhs_ref).astype(jnp.bfloat16).reshape(out_ref.shape)


def answer(lists, members, axis):
    senders, rows, lanes = lists.shape
    capacity = rows - META
    entries = senders * capacity
    step = math.gcd(members, 8)
    return pl.pallas_call(
        functools.partial(answer_kernel, axis, step),
        grid=(members // step,),
        out_shape=jax.ShapeDtypeStruct((members, capacity, lanes), jnp.bfloat16),
        in_specs=[vmem_spec()],
        out_specs=pl.BlockSpec((step, capacity, lanes), lambda i: (i, 0, 0)),
        scratch_shapes=[pltpu.VMEM((entries, 2 * lanes), jnp.bfloat16), pltpu.VMEM((1, entries), jnp.float32)],
        name="answer",
    )(lists)


def dense_kernel(lists_ref, out_ref, rhs_ref, key_ref):
    @pl.when(pl.program_id(0) == 0)
    def _():
        load_entries(lists_ref, rhs_ref, key_ref)

    tile = out_ref.shape[0]
    wanted = (lax.broadcasted_iota(jnp.int32, (tile, 1), 0) + pl.program_id(0) * tile).astype(jnp.float32)
    out_ref[...] = average(wanted, key_ref, rhs_ref)


def dense(lists):
    senders, rows, lanes = lists.shape
    capacity = rows - META
    entries = senders * capacity
    tile = math.gcd(BUCKET, 512)
    return pl.pallas_call(
        dense_kernel,
        grid=(BUCKET // tile,),
        out_shape=jax.ShapeDtypeStruct((BUCKET, lanes), jnp.float32),
        in_specs=[vmem_spec()],
        out_specs=pl.BlockSpec((tile, lanes), lambda i: (i, 0)),
        scratch_shapes=[pltpu.VMEM((entries, 2 * lanes), jnp.bfloat16), pltpu.VMEM((1, entries), jnp.float32)],
        cost_estimate=pl.CostEstimate(flops=4 * BUCKET * entries * lanes, bytes_accessed=4 * BUCKET * lanes, transcendentals=0),
        name="dense",
    )(lists)


def per_device(groups, values, slots, counts):
    members = values.shape[1]
    lists = pack(values[0], slots[0], counts, groups)
    got = lax.all_to_all(lists, ("grp", "mem"), split_axis=0, concat_axis=0, tiled=True)
    back = answer(got, members, "grp")
    returned = lax.all_to_all(back, "mem", split_axis=0, concat_axis=0, tiled=True)
    averaged = dense(got)
    return (averaged, returned[None])


def solution(mesh):
    return jax.shard_map(
        functools.partial(per_device, mesh.shape["grp"]),
        mesh=mesh,
        in_specs=(
            P(("grp", "mem"), None, None, None),
            P(("grp", "mem"), None, None),
            P(("grp", "mem"), None),
        ),
        out_specs=(P("mem", None), P(("grp", "mem"), None, None, None)),
        check_vma=False,
    )
```

```python
import functools
import math

import jax
import jax.numpy as jnp
from jax import lax
from jax.experimental import pallas as pl
from jax.experimental.pallas import tpu as pltpu
from jax.sharding import PartitionSpec as P

BUCKET = 7168
DIGIT = 256
META = 8


def vmem_spec():
    return pl.BlockSpec(memory_space=pltpu.VMEM)


def grant(size):
    return pltpu.CompilerParams(vmem_limit_bytes=size)


def pack_kernel(groups, values_ref, slots_ref, counts_ref, out_ref):
    members, capacity, lanes = values_ref.shape
    shape = (members, members)
    diagonal = lax.broadcasted_iota(jnp.int32, shape, 0) == lax.broadcasted_iota(jnp.int32, shape, 1)
    count = jnp.sum(jnp.where(diagonal, counts_ref[...].astype(jnp.float32), 0.0), axis=1, keepdims=True)
    slot = slots_ref[...]
    place = lax.broadcasted_iota(jnp.int32, slot.shape, 1).astype(jnp.float32)
    live = place < count
    high = jnp.where(live, (slot // DIGIT).astype(jnp.float32), -1.0)
    low = jnp.where(live, (slot % DIGIT).astype(jnp.float32), 0.0)
    repeats = lanes // capacity
    high = jnp.concatenate([high] * repeats, axis=1)
    low = jnp.concatenate([low] * repeats, axis=1)
    row = lax.broadcasted_iota(jnp.int32, (members, META, lanes), 1)
    meta = jnp.where(row == 0, high[:, None, :], jnp.where(row == 1, low[:, None, :], 0.0))
    meta = meta.astype(jnp.bfloat16)
    for group in range(groups):
        rows = pl.ds(group * members, members)
        out_ref[rows, pl.ds(0, capacity), :] = values_ref[...]
        out_ref[rows, pl.ds(capacity, META), :] = meta


def pack(values, slots, counts, groups):
    members, capacity, lanes = values.shape
    return pl.pallas_call(
        functools.partial(pack_kernel, groups),
        out_shape=jax.ShapeDtypeStruct((groups * members, capacity + META, lanes), jnp.bfloat16),
        in_specs=[vmem_spec()] * 3,
        out_specs=vmem_spec(),
        compiler_params=grant(8 * 2**20),
        name="pack",
    )(values, slots, counts)


def digits_of(lists_ref, first, senders):
    capacity = lists_ref.shape[1] - META
    meta = lists_ref[pl.ds(first, senders), pl.ds(capacity, META), :].astype(jnp.float32)
    return meta[:, 0, :], meta[:, 1, :]


def as_row(digit, capacity):
    senders, lanes = digit.shape
    per_block = lanes // capacity
    part = lax.broadcasted_iota(jnp.int32, (1, lanes), 1) // capacity
    blocks = []
    for block in range(senders // per_block):
        row = digit[block * per_block : block * per_block + 1]
        for k in range(1, per_block):
            at = block * per_block + k
            row = jnp.where(part == k, digit[at : at + 1], row)
        blocks.append(row)
    return jnp.concatenate(blocks, axis=1)


def as_column(digit, capacity):
    senders, lanes = digit.shape
    shape = (senders, capacity, lanes)
    here = lax.broadcasted_iota(jnp.int32, shape, 2) == lax.broadcasted_iota(jnp.int32, shape, 1)
    picked = jnp.where(here, digit[:, None, :], 0.0).astype(jnp.bfloat16).reshape(senders * capacity, lanes)
    return jnp.dot(picked, jnp.ones((lanes, lanes), jnp.bfloat16), preferred_element_type=jnp.float32)


def load_keys(lists_ref, key_ref):
    senders, rows, lanes = lists_ref.shape
    high, low = digits_of(lists_ref, 0, senders)
    key_ref[...] = as_row(high * DIGIT + low, rows - META)


def load_entries(lists_ref, rhs_ref, key_ref):
    senders, rows, lanes = lists_ref.shape
    capacity = rows - META
    load_keys(lists_ref, key_ref)
    rhs_ref[:, :lanes] = lists_ref[:, pl.ds(0, capacity), :].reshape(senders * capacity, lanes)
    rhs_ref[:, lanes:] = jnp.ones((senders * capacity, lanes), jnp.bfloat16)


def average(wanted, key_ref, rhs_ref):
    lanes = rhs_ref.shape[1] // 2
    onehot = (wanted == key_ref[...]).astype(jnp.float32).astype(jnp.bfloat16)
    both = jnp.dot(onehot, rhs_ref[...], preferred_element_type=jnp.float32)
    return both[:, :lanes] / jnp.maximum(both[:, lanes:], 1.0)


def answer_kernel(axis, step, lists_ref, out_ref, key_ref):
    senders, rows, lanes = lists_ref.shape
    capacity = rows - META

    @pl.when(pl.program_id(0) == 0)
    def _():
        load_keys(lists_ref, key_ref)

    members = step * pl.num_programs(0)
    first = lax.axis_index(axis) * members + pl.program_id(0) * step
    high, low = digits_of(lists_ref, first, step)
    column = as_column(high, capacity) * DIGIT + as_column(low, capacity)
    column = jnp.where(column < 0.0, -1.0, column)
    onehot = jnp.concatenate(
        [
            (column == key_ref[:, at : at + lanes]).astype(jnp.float32).astype(jnp.bfloat16)
            for at in range(0, senders * capacity, lanes)
        ],
        axis=1,
    )
    entries = lists_ref[:, pl.ds(0, capacity), :].reshape(senders * capacity, lanes)
    sums = jnp.dot(onehot, entries, preferred_element_type=jnp.float32)
    count = jnp.dot(onehot, jnp.ones_like(entries), preferred_element_type=jnp.float32)
    mean = sums / jnp.maximum(count, 1.0)
    out_ref[...] = mean.astype(jnp.bfloat16).reshape(out_ref.shape)


def answer(lists, members, axis):
    senders, rows, lanes = lists.shape
    capacity = rows - META
    entries = senders * capacity
    step = math.gcd(members, 8)
    return pl.pallas_call(
        functools.partial(answer_kernel, axis, step),
        grid=(members // step,),
        out_shape=jax.ShapeDtypeStruct((members, capacity, lanes), jnp.bfloat16),
        in_specs=[vmem_spec()],
        out_specs=pl.BlockSpec((step, capacity, lanes), lambda i: (i, 0, 0)),
        scratch_shapes=[pltpu.VMEM((1, entries), jnp.float32)],
        compiler_params=grant(48 * entries * lanes),
        name="answer",
    )(lists)


def dense_kernel(lists_ref, out_ref, rhs_ref, key_ref):
    @pl.when(pl.program_id(0) == 0)
    def _():
        load_entries(lists_ref, rhs_ref, key_ref)

    tile = out_ref.shape[0]
    wanted = (lax.broadcasted_iota(jnp.int32, (tile, 1), 0) + pl.program_id(0) * tile).astype(jnp.float32)
    out_ref[...] = average(wanted, key_ref, rhs_ref)


def dense_whole_kernel(lists_ref, out_ref, same_ref, high_ref, mean_ref, sems):
    senders, rows, lanes = lists_ref.shape
    capacity = rows - META
    entries = senders * capacity
    high, low = digits_of(lists_ref, 0, senders)
    low_row = as_row(low, capacity)
    wanted = lax.broadcasted_iota(jnp.int32, (DIGIT, lanes), 0).astype(jnp.float32)
    for at in range(0, entries, lanes):
        same = (wanted == low_row[:, at : at + lanes]).astype(jnp.float32)
        same_ref[:, at : at + lanes] = same.astype(jnp.bfloat16)
    high_column = as_column(high, capacity)
    high_ref[...] = high_column.astype(jnp.bfloat16)
    lane = lax.broadcasted_iota(jnp.int32, (entries, lanes), 1).astype(jnp.float32)
    in_tile = (high_column == lane).astype(jnp.float32).astype(jnp.bfloat16)
    count = jnp.dot(same_ref[...], in_tile, preferred_element_type=jnp.float32)
    inverse = 1.0 / jnp.maximum(count, 1.0)
    copies = []
    for pair in range(BUCKET // (2 * DIGIT)):
        values = lists_ref[:, pl.ds(0, capacity), :].reshape(entries, lanes)
        tile_of = high_ref[...]
        zero = jnp.zeros_like(values)
        picked = jnp.concatenate([jnp.where(tile_of == 2 * pair + k, values, zero) for k in range(2)], axis=1)
        sums = jnp.dot(same_ref[...], picked, preferred_element_type=jnp.float32)
        for k in range(2):
            tile = 2 * pair + k
            where = pl.ds(tile * DIGIT, DIGIT)
            mean_ref[where, :] = sums[:, k * lanes : (k + 1) * lanes] * inverse[:, tile : tile + 1]
        where = pl.ds(2 * pair * DIGIT, 2 * DIGIT)
        copy = pltpu.make_async_copy(mean_ref.at[where], out_ref.at[where], sems.at[pair])
        copy.start()
        copies.append(copy)
    for copy in copies:
        copy.wait()


def dense_whole(lists):
    senders, rows, lanes = lists.shape
    entries = senders * (rows - META)
    return pl.pallas_call(
        dense_whole_kernel,
        out_shape=jax.ShapeDtypeStruct((BUCKET, lanes), jnp.float32),
        in_specs=[vmem_spec()],
        out_specs=pl.BlockSpec(memory_space=pltpu.HBM),
        scratch_shapes=[
            pltpu.VMEM((DIGIT, entries), jnp.bfloat16),
            pltpu.VMEM((entries, lanes), jnp.bfloat16),
            pltpu.VMEM((BUCKET, lanes), jnp.float32),
            pltpu.SemaphoreType.DMA((BUCKET // (2 * DIGIT),)),
        ],
        cost_estimate=dense_cost(entries, lanes),
        compiler_params=grant(16 * 2**20),
        name="dense_whole",
    )(lists)


def dense_cost(entries, lanes):
    return pl.CostEstimate(flops=2 * BUCKET * entries * lanes, bytes_accessed=4 * BUCKET * lanes, transcendentals=0)


def dense(lists):
    senders, rows, lanes = lists.shape
    capacity = rows - META
    entries = senders * capacity
    if entries <= 1024 and BUCKET % (2 * DIGIT) == 0 and BUCKET // DIGIT <= lanes:
        return dense_whole(lists)
    tile = math.gcd(BUCKET, 512)
    return pl.pallas_call(
        dense_kernel,
        grid=(BUCKET // tile,),
        out_shape=jax.ShapeDtypeStruct((BUCKET, lanes), jnp.float32),
        in_specs=[vmem_spec()],
        out_specs=pl.BlockSpec((tile, lanes), lambda i: (i, 0)),
        scratch_shapes=[pltpu.VMEM((entries, 2 * lanes), jnp.bfloat16), pltpu.VMEM((1, entries), jnp.float32)],
        cost_estimate=dense_cost(entries, lanes),
        name="dense",
    )(lists)


def per_device(groups, values, slots, counts):
    members = values.shape[1]
    lists = pack(values[0], slots[0], counts, groups)
    got = lax.all_to_all(lists, ("grp", "mem"), split_axis=0, concat_axis=0, tiled=True)
    back = answer(got, members, "grp")
    returned = lax.all_to_all(back, "mem", split_axis=0, concat_axis=0, tiled=True)
    averaged = dense(got)
    return (averaged, returned[None])


def solution(mesh):
    return jax.shard_map(
        functools.partial(per_device, mesh.shape["grp"]),
        mesh=mesh,
        in_specs=(
            P(("grp", "mem"), None, None, None),
            P(("grp", "mem"), None, None),
            P(("grp", "mem"), None),
        ),
        out_specs=(P("mem", None), P(("grp", "mem"), None, None, None)),
        check_vma=False,
    )
```

```python
import functools
import math

import jax
import jax.numpy as jnp
from jax import lax
from jax.experimental import pallas as pl
from jax.experimental.pallas import tpu as pltpu
from jax.sharding import PartitionSpec as P

BUCKET = 7168
DIGIT = 256
META = 8


def vmem_spec():
    return pl.BlockSpec(memory_space=pltpu.VMEM)


def hbm_spec():
    return pl.BlockSpec(memory_space=pltpu.HBM)


def grant(size):
    return pltpu.CompilerParams(vmem_limit_bytes=size)


def pack_kernel(groups, values_ref, high_ref, low_ref, out_ref):
    members, capacity, lanes = values_ref.shape
    repeats = lanes // capacity
    high = jnp.concatenate([high_ref[...]] * repeats, axis=1)
    low = jnp.concatenate([low_ref[...]] * repeats, axis=1)
    row = lax.broadcasted_iota(jnp.int32, (members, META, lanes), 1)
    meta = jnp.where(row == 0, high[:, None, :], low[:, None, :]).astype(jnp.bfloat16)
    for group in range(groups):
        rows = pl.ds(group * members, members)
        out_ref[rows, pl.ds(0, capacity), :] = values_ref[...]
        out_ref[rows, pl.ds(capacity, META), :] = meta


def pack(values, slots, counts, groups):
    members, capacity, lanes = values.shape
    live = lax.broadcasted_iota(jnp.int32, slots.shape, 1) < counts[:, None]
    high = jnp.where(live, slots // DIGIT, -1).astype(jnp.float32)
    low = jnp.where(live, slots % DIGIT, 0).astype(jnp.float32)
    return pl.pallas_call(
        functools.partial(pack_kernel, groups),
        out_shape=jax.ShapeDtypeStruct((groups * members, capacity + META, lanes), jnp.bfloat16),
        in_specs=[vmem_spec()] * 3,
        out_specs=vmem_spec(),
        compiler_params=grant(8 * 2**20),
        name="pack",
    )(values, high, low)


def digits_of(lists_ref, first, senders):
    capacity = lists_ref.shape[1] - META
    meta = lists_ref[pl.ds(first, senders), pl.ds(capacity, META), :].astype(jnp.float32)
    return meta[:, 0, :], meta[:, 1, :]


def as_row(digit, capacity):
    senders, lanes = digit.shape
    per_block = lanes // capacity
    part = lax.broadcasted_iota(jnp.int32, (1, lanes), 1) // capacity
    blocks = []
    for block in range(senders // per_block):
        row = digit[block * per_block : block * per_block + 1]
        for k in range(1, per_block):
            at = block * per_block + k
            row = jnp.where(part == k, digit[at : at + 1], row)
        blocks.append(row)
    return jnp.concatenate(blocks, axis=1)


def as_column(digit, capacity):
    senders, lanes = digit.shape
    shape = (senders, capacity, lanes)
    here = lax.broadcasted_iota(jnp.int32, shape, 2) == lax.broadcasted_iota(jnp.int32, shape, 1)
    picked = jnp.where(here, digit[:, None, :], 0.0).astype(jnp.bfloat16).reshape(senders * capacity, lanes)
    return jnp.dot(picked, jnp.ones((lanes, lanes), jnp.bfloat16), preferred_element_type=jnp.float32)


def load_keys(lists_ref, key_ref):
    senders, rows, lanes = lists_ref.shape
    high, low = digits_of(lists_ref, 0, senders)
    key_ref[...] = as_row(high * DIGIT + low, rows - META)


def load_entries(lists_ref, rhs_ref, key_ref):
    senders, rows, lanes = lists_ref.shape
    capacity = rows - META
    load_keys(lists_ref, key_ref)
    rhs_ref[:, :lanes] = lists_ref[:, pl.ds(0, capacity), :].reshape(senders * capacity, lanes)
    rhs_ref[:, lanes:] = jnp.ones((senders * capacity, lanes), jnp.bfloat16)


def average(wanted, key_ref, rhs_ref):
    lanes = rhs_ref.shape[1] // 2
    onehot = (wanted == key_ref[...]).astype(jnp.float32).astype(jnp.bfloat16)
    both = jnp.dot(onehot, rhs_ref[...], preferred_element_type=jnp.float32)
    return both[:, :lanes] / jnp.maximum(both[:, lanes:], 1.0)


def answer_some(lists_ref, key_ref, asking):
    senders, rows, lanes = lists_ref.shape
    capacity = rows - META
    digits = [digits_of(lists_ref, at, 1) for at in asking]
    high = jnp.concatenate([pair[0] for pair in digits], axis=0)
    low = jnp.concatenate([pair[1] for pair in digits], axis=0)
    column = as_column(high, capacity) * DIGIT + as_column(low, capacity)
    column = jnp.where(column < 0.0, -1.0, column)
    onehot = jnp.concatenate(
        [
            (column == key_ref[:, block : block + lanes]).astype(jnp.float32).astype(jnp.bfloat16)
            for block in range(0, senders * capacity, lanes)
        ],
        axis=1,
    )
    entries = lists_ref[:, pl.ds(0, capacity), :].reshape(senders * capacity, lanes)
    sums = jnp.dot(onehot, entries, preferred_element_type=jnp.float32)
    count = jnp.dot(onehot, jnp.ones_like(entries), preferred_element_type=jnp.float32)
    mean = sums / jnp.maximum(count, 1.0)
    return mean.astype(jnp.bfloat16).reshape(len(asking), capacity, lanes)


def answer_kernel(lists_ref, out_ref, key_ref):
    members = out_ref.shape[0]
    step = math.gcd(members, 8)
    load_keys(lists_ref, key_ref)
    first = lax.axis_index("grp") * members

    @pl.loop(0, members, step=step)
    def _(at):
        asking = [first + at + k for k in range(step)]
        out_ref[pl.ds(at, step)] = answer_some(lists_ref, key_ref, asking)


def pair_answer_kernel(lists_ref, same_ref, other_ref, key_ref):
    pairs = same_ref.shape[0]
    load_keys(lists_ref, key_ref)
    first = lax.axis_index("grp") * 2 * pairs
    me = lax.axis_index("mem")
    half = lax.rem(me, 2)
    pair = lax.div(me, 2)
    order = [first + 2 * lax.rem(pair + k, pairs) for k in range(pairs)]
    asking = [at + half for at in order] + [at + 1 - half for at in order]
    both = answer_some(lists_ref, key_ref, asking)
    same_ref[...] = both[:pairs]
    other_ref[...] = both[pairs:]


def answer(lists, members, paired):
    senders, rows, lanes = lists.shape
    capacity = rows - META
    entries = senders * capacity
    parts = 2 if paired else 1
    return pl.pallas_call(
        pair_answer_kernel if paired else answer_kernel,
        out_shape=[jax.ShapeDtypeStruct((members // parts, capacity, lanes), jnp.bfloat16)] * parts,
        in_specs=[vmem_spec()],
        out_specs=[vmem_spec()] * parts,
        scratch_shapes=[pltpu.VMEM((1, entries), jnp.float32)],
        compiler_params=grant(48 * entries * lanes),
        name="answer",
    )(lists)


def place_kernel(*refs):
    *parts, out_ref, sems = refs
    pairs = out_ref.shape[0] // 2
    me = lax.axis_index("mem")
    half = lax.rem(me, 2)
    pair = lax.div(me, 2)
    copies = []
    for k in range(pairs):
        source = 2 * lax.rem(pair + pairs - k, pairs)
        two = (parts[0].at[0], parts[1].at[0]) if k == 0 else (parts[k + 1].at[0], parts[k + 1].at[1])
        for part, at in zip(two, (source + half, source + 1 - half)):
            copies.append(pltpu.make_async_copy(part, out_ref.at[at], sems.at[len(copies)]))
    for copy in copies:
        copy.start()
    for copy in copies:
        copy.wait()


def place(parts, members):
    capacity, lanes = parts[0].shape[1:]
    return pl.pallas_call(
        place_kernel,
        out_shape=jax.ShapeDtypeStruct((members, capacity, lanes), jnp.bfloat16),
        in_specs=[vmem_spec()] * len(parts),
        out_specs=hbm_spec(),
        scratch_shapes=[pltpu.SemaphoreType.DMA((members,))],
        compiler_params=grant(2 * 2**20),
        name="place",
    )(*parts)


def send_back(lists, members):
    if members % 2 or members > 8:
        (back,) = answer(lists, members, False)
        return lax.all_to_all(back, "mem", split_axis=0, concat_axis=0, tiled=True)
    same, other = answer(lists, members, True)
    mine = lax.ppermute(other, "mem", [(i, i ^ 1) for i in range(members)])
    parts = [same, mine]
    for k in range(1, members // 2):
        two = jnp.concatenate([same[k : k + 1], mine[k : k + 1]], axis=0)
        parts.append(lax.ppermute(two, "mem", [(i, (i + 2 * k) % members) for i in range(members)]))
    return place(parts, members)


def dense_kernel(lists_ref, out_ref, rhs_ref, key_ref):
    @pl.when(pl.program_id(0) == 0)
    def _():
        load_entries(lists_ref, rhs_ref, key_ref)

    tile = out_ref.shape[0]
    wanted = (lax.broadcasted_iota(jnp.int32, (tile, 1), 0) + pl.program_id(0) * tile).astype(jnp.float32)
    out_ref[...] = average(wanted, key_ref, rhs_ref)


def dense_whole_kernel(lists_ref, out_ref, same_ref, high_ref, mean_ref, sems):
    senders, rows, lanes = lists_ref.shape
    capacity = rows - META
    entries = senders * capacity
    high, low = digits_of(lists_ref, 0, senders)
    low_row = as_row(low, capacity)
    wanted = lax.broadcasted_iota(jnp.int32, (DIGIT, lanes), 0).astype(jnp.float32)
    for at in range(0, entries, lanes):
        same = (wanted == low_row[:, at : at + lanes]).astype(jnp.float32)
        same_ref[:, at : at + lanes] = same.astype(jnp.bfloat16)
    high_column = as_column(high, capacity)
    high_ref[...] = high_column.astype(jnp.bfloat16)
    lane = lax.broadcasted_iota(jnp.int32, (entries, lanes), 1).astype(jnp.float32)
    in_tile = (high_column == lane).astype(jnp.float32).astype(jnp.bfloat16)
    count = jnp.dot(same_ref[...], in_tile, preferred_element_type=jnp.float32)
    inverse = 1.0 / jnp.maximum(count, 1.0)
    copies = []
    for pair in range(BUCKET // (2 * DIGIT)):
        values = lists_ref[:, pl.ds(0, capacity), :].reshape(entries, lanes)
        tile_of = high_ref[...]
        zero = jnp.zeros_like(values)
        picked = jnp.concatenate([jnp.where(tile_of == 2 * pair + k, values, zero) for k in range(2)], axis=1)
        sums = jnp.dot(same_ref[...], picked, preferred_element_type=jnp.float32)
        for k in range(2):
            tile = 2 * pair + k
            where = pl.ds(tile * DIGIT, DIGIT)
            mean_ref[where, :] = sums[:, k * lanes : (k + 1) * lanes] * inverse[:, tile : tile + 1]
        where = pl.ds(2 * pair * DIGIT, 2 * DIGIT)
        copy = pltpu.make_async_copy(mean_ref.at[where], out_ref.at[where], sems.at[pair])
        copy.start()
        copies.append(copy)
    for copy in copies:
        copy.wait()


def dense_whole(lists):
    senders, rows, lanes = lists.shape
    entries = senders * (rows - META)
    return pl.pallas_call(
        dense_whole_kernel,
        out_shape=jax.ShapeDtypeStruct((BUCKET, lanes), jnp.float32),
        in_specs=[vmem_spec()],
        out_specs=hbm_spec(),
        scratch_shapes=[
            pltpu.VMEM((DIGIT, entries), jnp.bfloat16),
            pltpu.VMEM((entries, lanes), jnp.bfloat16),
            pltpu.VMEM((BUCKET, lanes), jnp.float32),
            pltpu.SemaphoreType.DMA((BUCKET // (2 * DIGIT),)),
        ],
        cost_estimate=dense_cost(entries, lanes),
        compiler_params=grant(16 * 2**20),
        name="dense_whole",
    )(lists)


def dense_cost(entries, lanes):
    return pl.CostEstimate(flops=2 * BUCKET * entries * lanes, bytes_accessed=4 * BUCKET * lanes, transcendentals=0)


def dense(lists):
    senders, rows, lanes = lists.shape
    capacity = rows - META
    entries = senders * capacity
    if entries <= 1024 and BUCKET % (2 * DIGIT) == 0 and BUCKET // DIGIT <= lanes:
        return dense_whole(lists)
    tile = math.gcd(BUCKET, 512)
    return pl.pallas_call(
        dense_kernel,
        grid=(BUCKET // tile,),
        out_shape=jax.ShapeDtypeStruct((BUCKET, lanes), jnp.float32),
        in_specs=[vmem_spec()],
        out_specs=pl.BlockSpec((tile, lanes), lambda i: (i, 0)),
        scratch_shapes=[pltpu.VMEM((entries, 2 * lanes), jnp.bfloat16), pltpu.VMEM((1, entries), jnp.float32)],
        cost_estimate=dense_cost(entries, lanes),
        name="dense",
    )(lists)


def per_device(groups, values, slots, counts):
    members = values.shape[1]
    lists = pack(values[0], slots[0], counts[0], groups)
    got = lax.all_to_all(lists, ("grp", "mem"), split_axis=0, concat_axis=0, tiled=True)
    returned = send_back(got, members)
    averaged = dense(got)
    return (averaged, returned[None])


def solution(mesh):
    return jax.shard_map(
        functools.partial(per_device, mesh.shape["grp"]),
        mesh=mesh,
        in_specs=(
            P(("grp", "mem"), None, None, None),
            P(("grp", "mem"), None, None),
            P(("grp", "mem"), None),
        ),
        out_specs=(P("mem", None), P(("grp", "mem"), None, None, None)),
        check_vma=False,
    )
```

```python
import functools
import math

import jax
import jax.numpy as jnp
from jax import lax
from jax.experimental import pallas as pl
from jax.experimental.pallas import tpu as pltpu
from jax.sharding import PartitionSpec as P

BUCKET = 7168
DIGIT = 256
TILE = 512
META = 8


def vmem_spec():
    return pl.BlockSpec(memory_space=pltpu.VMEM)


def hbm_spec():
    return pl.BlockSpec(memory_space=pltpu.HBM)


def grant(size):
    return pltpu.CompilerParams(vmem_limit_bytes=size)


def place_in_list_kernel(out_ref):
    out_ref[...] = lax.broadcasted_iota(jnp.int32, out_ref.shape, 1).astype(jnp.float32)


def pack_kernel(groups, values_ref, slots_ref, counts_ref, place_ref, out_ref):
    members, capacity, lanes = values_ref.shape
    shape = (members, members)
    diagonal = lax.broadcasted_iota(jnp.int32, shape, 0) == lax.broadcasted_iota(jnp.int32, shape, 1)
    count = jnp.sum(jnp.where(diagonal, counts_ref[...].astype(jnp.float32), 0.0), axis=1, keepdims=True)
    slot = slots_ref[...]
    live = place_ref[...] < count
    high = jnp.where(live, (slot // DIGIT).astype(jnp.float32), -1.0)
    low = jnp.where(live, (slot % DIGIT).astype(jnp.float32), 0.0)
    repeats = lanes // capacity
    high = jnp.concatenate([high] * repeats, axis=1)
    low = jnp.concatenate([low] * repeats, axis=1)
    row = lax.broadcasted_iota(jnp.int32, (members, META, lanes), 1)
    meta = jnp.where(row == 0, high[:, None, :], low[:, None, :]).astype(jnp.bfloat16)
    for group in range(groups):
        rows = pl.ds(group * members, members)
        out_ref[rows, pl.ds(0, capacity), :] = values_ref[...]
        out_ref[rows, pl.ds(capacity, META), :] = meta


def pack(values, slots, counts, groups):
    members, capacity, lanes = values.shape
    place_in_list = pl.pallas_call(
        place_in_list_kernel,
        out_shape=jax.ShapeDtypeStruct(slots.shape, jnp.float32),
        out_specs=vmem_spec(),
        cost_estimate=pl.CostEstimate(flops=2 * 10**9, bytes_accessed=16 * 10**6, transcendentals=0),
        compiler_params=grant(2**20),
        name="place_in_list",
    )()
    return pl.pallas_call(
        functools.partial(pack_kernel, groups),
        out_shape=jax.ShapeDtypeStruct((groups * members, capacity + META, lanes), jnp.bfloat16),
        in_specs=[vmem_spec()] * 4,
        out_specs=vmem_spec(),
        compiler_params=grant(8 * 2**20),
        name="pack",
    )(values, slots, counts, place_in_list)


def digits_of(lists_ref, first, senders):
    capacity = lists_ref.shape[1] - META
    meta = lists_ref[pl.ds(first, senders), pl.ds(capacity, META), :].astype(jnp.float32)
    return meta[:, 0, :], meta[:, 1, :]


def as_row(digit, capacity):
    senders, lanes = digit.shape
    per_block = lanes // capacity
    part = lax.broadcasted_iota(jnp.int32, (1, lanes), 1) // capacity
    blocks = []
    for block in range(senders // per_block):
        row = digit[block * per_block : block * per_block + 1]
        for k in range(1, per_block):
            at = block * per_block + k
            row = jnp.where(part == k, digit[at : at + 1], row)
        blocks.append(row)
    return jnp.concatenate(blocks, axis=1)


def as_column(digit, capacity):
    senders, lanes = digit.shape
    shape = (senders, capacity, lanes)
    here = lax.broadcasted_iota(jnp.int32, shape, 2) == lax.broadcasted_iota(jnp.int32, shape, 1)
    picked = jnp.where(here, digit[:, None, :], 0.0).astype(jnp.bfloat16).reshape(senders * capacity, lanes)
    return jnp.dot(picked, jnp.ones((lanes, lanes), jnp.bfloat16), preferred_element_type=jnp.float32)


def load_keys(lists_ref, key_ref):
    senders, rows, lanes = lists_ref.shape
    high, low = digits_of(lists_ref, 0, senders)
    key_ref[...] = as_row(high * DIGIT + low, rows - META)


def load_entries(lists_ref, rhs_ref, key_ref):
    senders, rows, lanes = lists_ref.shape
    capacity = rows - META
    load_keys(lists_ref, key_ref)
    rhs_ref[:, :lanes] = lists_ref[:, pl.ds(0, capacity), :].reshape(senders * capacity, lanes)
    rhs_ref[:, lanes:] = jnp.ones((senders * capacity, lanes), jnp.bfloat16)


def average(wanted, key_ref, rhs_ref):
    lanes = rhs_ref.shape[1] // 2
    onehot = (wanted == key_ref[...]).astype(jnp.float32).astype(jnp.bfloat16)
    both = jnp.dot(onehot, rhs_ref[...], preferred_element_type=jnp.float32)
    return both[:, :lanes] / jnp.maximum(both[:, lanes:], 1.0)


def answer_some(lists_ref, key_ref, asking):
    senders, rows, lanes = lists_ref.shape
    capacity = rows - META
    digits = [digits_of(lists_ref, at, 1) for at in asking]
    high = jnp.concatenate([pair[0] for pair in digits], axis=0)
    low = jnp.concatenate([pair[1] for pair in digits], axis=0)
    column = as_column(high, capacity) * DIGIT + as_column(low, capacity)
    column = jnp.where(column < 0.0, -1.0, column)
    onehot = jnp.concatenate(
        [
            (column == key_ref[:, block : block + lanes]).astype(jnp.float32).astype(jnp.bfloat16)
            for block in range(0, senders * capacity, lanes)
        ],
        axis=1,
    )
    entries = lists_ref[:, pl.ds(0, capacity), :].reshape(senders * capacity, lanes)
    sums = jnp.dot(onehot, entries, preferred_element_type=jnp.float32)
    count = jnp.dot(onehot, jnp.ones_like(entries), preferred_element_type=jnp.float32)
    mean = sums / jnp.maximum(count, 1.0)
    return mean.astype(jnp.bfloat16).reshape(len(asking), capacity, lanes)


def answer_kernel(lists_ref, out_ref, key_ref):
    members = out_ref.shape[0]
    step = math.gcd(members, 8)
    load_keys(lists_ref, key_ref)
    first = lax.axis_index("grp") * members

    @pl.loop(0, members, step=step)
    def _(at):
        asking = [first + at + k for k in range(step)]
        out_ref[pl.ds(at, step)] = answer_some(lists_ref, key_ref, asking)


def pair_answer_kernel(lists_ref, same_ref, other_ref, key_ref):
    pairs = same_ref.shape[0]
    load_keys(lists_ref, key_ref)
    first = lax.axis_index("grp") * 2 * pairs
    me = lax.axis_index("mem")
    half = lax.rem(me, 2)
    pair = lax.div(me, 2)
    order = [first + 2 * lax.rem(pair + k, pairs) for k in range(pairs)]
    asking = [at + half for at in order] + [at + 1 - half for at in order]
    both = answer_some(lists_ref, key_ref, asking)
    same_ref[...] = both[:pairs]
    other_ref[...] = both[pairs:]


def answer(lists, members, paired):
    senders, rows, lanes = lists.shape
    capacity = rows - META
    entries = senders * capacity
    parts = 2 if paired else 1
    return pl.pallas_call(
        pair_answer_kernel if paired else answer_kernel,
        out_shape=[jax.ShapeDtypeStruct((members // parts, capacity, lanes), jnp.bfloat16)] * parts,
        in_specs=[vmem_spec()],
        out_specs=[vmem_spec()] * parts,
        scratch_shapes=[pltpu.VMEM((1, entries), jnp.float32)],
        compiler_params=grant(48 * entries * lanes),
        name="answer",
    )(lists)


def place_kernel(*refs):
    *parts, out_ref, sems = refs
    pairs = out_ref.shape[0] // 2
    me = lax.axis_index("mem")
    half = lax.rem(me, 2)
    pair = lax.div(me, 2)
    copies = []
    for k in range(pairs):
        source = 2 * lax.rem(pair + pairs - k, pairs)
        two = (parts[0].at[0], parts[1].at[0]) if k == 0 else (parts[k + 1].at[0], parts[k + 1].at[1])
        for part, at in zip(two, (source + half, source + 1 - half)):
            copies.append(pltpu.make_async_copy(part, out_ref.at[at], sems.at[len(copies)]))
    for copy in copies:
        copy.start()
    for copy in copies:
        copy.wait()


def place(parts, members):
    capacity, lanes = parts[0].shape[1:]
    return pl.pallas_call(
        place_kernel,
        out_shape=jax.ShapeDtypeStruct((members, capacity, lanes), jnp.bfloat16),
        in_specs=[vmem_spec()] * len(parts),
        out_specs=hbm_spec(),
        scratch_shapes=[pltpu.SemaphoreType.DMA((members,))],
        compiler_params=grant(2 * 2**20),
        name="place",
    )(*parts)


def send_back(lists, members):
    if members % 2 or members > 8:
        (back,) = answer(lists, members, False)
        return lax.all_to_all(back, "mem", split_axis=0, concat_axis=0, tiled=True)
    same, other = answer(lists, members, True)
    mine = lax.ppermute(other, "mem", [(i, i ^ 1) for i in range(members)])
    parts = [same, mine]
    for k in range(1, members // 2):
        two = jnp.concatenate([same[k : k + 1], mine[k : k + 1]], axis=0)
        parts.append(lax.ppermute(two, "mem", [(i, (i + 2 * k) % members) for i in range(members)]))
    return place(parts, members)


def dense_kernel(lists_ref, out_ref, rhs_ref, key_ref):
    @pl.when(pl.program_id(0) == 0)
    def _():
        load_entries(lists_ref, rhs_ref, key_ref)

    tile = out_ref.shape[0]
    wanted = (lax.broadcasted_iota(jnp.int32, (tile, 1), 0) + pl.program_id(0) * tile).astype(jnp.float32)
    out_ref[...] = average(wanted, key_ref, rhs_ref)


def tile_pair(pair, lists_ref, same_ref, tile_ref, inverse_ref, mean_ref, out_ref, sem):
    senders, rows, lanes = lists_ref.shape
    capacity = rows - META
    values = lists_ref[:, pl.ds(0, capacity), :].reshape(senders * capacity, lanes)
    tile_of = tile_ref[...]
    zero = jnp.zeros_like(values)
    picked = jnp.concatenate([jnp.where(tile_of == 2 * pair + k, values, zero) for k in range(2)], axis=1)
    sums = jnp.dot(same_ref[...], picked, preferred_element_type=jnp.float32)
    copies = []
    for k in range(2):
        tile = 2 * pair + k
        where = pl.ds(tile * TILE, TILE)
        part = mean_ref.at[pl.ds(k * TILE, TILE)]
        part[...] = sums[:, k * lanes : (k + 1) * lanes] * inverse_ref[:, tile : tile + 1]
        copy = pltpu.make_async_copy(part, out_ref.at[where], sem.at[k])
        copy.start()
        copies.append(copy)
    return copies


def dense_prepare_kernel(lists_ref, same_ref, tile_ref, inverse_ref):
    senders, rows, lanes = lists_ref.shape
    capacity = rows - META
    entries = senders * capacity
    ratio = TILE // DIGIT
    high, low = digits_of(lists_ref, 0, senders)
    tile = jnp.floor(high * (1.0 / ratio))
    low_row = as_row(low + DIGIT * (high - ratio * tile), capacity)
    wanted = lax.broadcasted_iota(jnp.int32, (TILE, lanes), 0).astype(jnp.float32)
    for at in range(0, entries, lanes):
        same = (wanted == low_row[:, at : at + lanes]).astype(jnp.float32)
        same_ref[:, at : at + lanes] = same.astype(jnp.bfloat16)
    tile_column = as_column(tile, capacity)
    tile_ref[...] = tile_column.astype(jnp.bfloat16)
    lane = lax.broadcasted_iota(jnp.int32, (entries, lanes), 1).astype(jnp.float32)
    in_tile = (tile_column == lane).astype(jnp.float32).astype(jnp.bfloat16)
    number = jnp.dot(same_ref[...], in_tile, preferred_element_type=jnp.float32)
    inverse_ref[...] = 1.0 / jnp.maximum(number, 1.0)


def dense_tiles_kernel(lists_ref, same_ref, tile_ref, inverse_ref, out_ref, mean_ref, sems):
    copies = []
    for pair in range(sems.shape[0]):
        part = mean_ref.at[pl.ds(2 * pair * TILE, 2 * TILE)]
        copies += tile_pair(pair, lists_ref, same_ref, tile_ref, inverse_ref, part, out_ref, sems.at[pair])
    for copy in copies:
        copy.wait()


def dense_split(lists):
    senders, rows, lanes = lists.shape
    entries = senders * (rows - META)
    same, tile, inverse = pl.pallas_call(
        dense_prepare_kernel,
        out_shape=[
            jax.ShapeDtypeStruct((TILE, entries), jnp.bfloat16),
            jax.ShapeDtypeStruct((entries, lanes), jnp.bfloat16),
            jax.ShapeDtypeStruct((TILE, lanes), jnp.float32),
        ],
        in_specs=[vmem_spec()],
        out_specs=[vmem_spec()] * 3,
        cost_estimate=dense_cost(entries, lanes, TILE / BUCKET),
        compiler_params=grant(8 * 2**20),
        name="dense_prepare",
    )(lists)
    return pl.pallas_call(
        dense_tiles_kernel,
        out_shape=jax.ShapeDtypeStruct((BUCKET, lanes), jnp.float32),
        in_specs=[vmem_spec()] * 4,
        out_specs=hbm_spec(),
        scratch_shapes=[
            pltpu.VMEM((BUCKET, lanes), jnp.float32),
            pltpu.SemaphoreType.DMA((BUCKET // (2 * TILE), 2)),
        ],
        cost_estimate=dense_cost(entries, lanes),
        compiler_params=grant(16 * 2**20),
        name="dense_tiles",
    )(lists, same, tile, inverse)


def dense_cost(entries, lanes, share=1.0):
    flops = int(2 * BUCKET * entries * lanes * share)
    return pl.CostEstimate(flops=flops, bytes_accessed=int(4 * BUCKET * lanes * share), transcendentals=0)


def dense(lists):
    senders, rows, lanes = lists.shape
    capacity = rows - META
    entries = senders * capacity
    if entries <= 1024 and BUCKET % (2 * TILE) == 0 and BUCKET // TILE <= lanes:
        return dense_split(lists)
    tile = math.gcd(BUCKET, 512)
    return pl.pallas_call(
        dense_kernel,
        grid=(BUCKET // tile,),
        out_shape=jax.ShapeDtypeStruct((BUCKET, lanes), jnp.float32),
        in_specs=[vmem_spec()],
        out_specs=pl.BlockSpec((tile, lanes), lambda i: (i, 0)),
        scratch_shapes=[pltpu.VMEM((entries, 2 * lanes), jnp.bfloat16), pltpu.VMEM((1, entries), jnp.float32)],
        cost_estimate=dense_cost(entries, lanes),
        name="dense",
    )(lists)


def per_device(groups, values, slots, counts):
    members = values.shape[1]
    lists = pack(values[0], slots[0], counts, groups)
    got = lax.all_to_all(lists, ("grp", "mem"), split_axis=0, concat_axis=0, tiled=True)
    returned = send_back(got, members)
    averaged = dense(got)
    return (averaged, returned[None])


def solution(mesh):
    return jax.shard_map(
        functools.partial(per_device, mesh.shape["grp"]),
        mesh=mesh,
        in_specs=(
            P(("grp", "mem"), None, None, None),
            P(("grp", "mem"), None, None),
            P(("grp", "mem"), None),
        ),
        out_specs=(P("mem", None), P(("grp", "mem"), None, None, None)),
        check_vma=False,
    )
```

```python
import functools
import math

import jax
import jax.numpy as jnp
from jax import lax
from jax.experimental import pallas as pl
from jax.experimental.pallas import tpu as pltpu
from jax.sharding import PartitionSpec as P


BUCKET = 7168
DIGIT = 256
TILE = 512
META = 8
MIB = 2**20


def vmem_spec():
    return pl.BlockSpec(memory_space=pltpu.VMEM)


def hbm_spec():
    return pl.BlockSpec(memory_space=pltpu.HBM)


def grant(size):
    return pltpu.CompilerParams(vmem_limit_bytes=size)


def lists_shape(count, capacity, lanes):
    return jax.ShapeDtypeStruct((count, capacity + META, lanes), jnp.bfloat16)


def place_in_list_kernel(out_ref):
    out_ref[...] = lax.broadcasted_iota(jnp.int32, out_ref.shape, 1).astype(jnp.float32)


def meta_rows(slots_ref, counts_ref, place_ref, lanes):
    members, capacity = slots_ref.shape
    shape = (members, members)
    diagonal = lax.broadcasted_iota(jnp.int32, shape, 0) == lax.broadcasted_iota(jnp.int32, shape, 1)
    count = jnp.sum(jnp.where(diagonal, counts_ref[...].astype(jnp.float32), 0.0), axis=1, keepdims=True)
    slot = slots_ref[...]
    live = place_ref[...] < count
    high = jnp.where(live, (slot // DIGIT).astype(jnp.float32), -1.0)
    low = jnp.where(live, (slot % DIGIT).astype(jnp.float32), 0.0)
    repeats = lanes // capacity
    high = jnp.concatenate([high] * repeats, axis=1)
    low = jnp.concatenate([low] * repeats, axis=1)
    row = lax.broadcasted_iota(jnp.int32, (members, META, lanes), 1)
    return jnp.where(row == 0, high[:, None, :], low[:, None, :]).astype(jnp.bfloat16)


def pack_groups_kernel(values_ref, slots_ref, counts_ref, place_ref, out_ref):
    members, capacity, lanes = values_ref.shape
    meta = meta_rows(slots_ref, counts_ref, place_ref, lanes)
    for group in range(out_ref.shape[0] // members):
        rows = pl.ds(group * members, members)
        out_ref[rows, pl.ds(0, capacity), :] = values_ref[...]
        out_ref[rows, pl.ds(capacity, META), :] = meta


def pack_pairs_kernel(values_ref, slots_ref, counts_ref, place_ref, *out_and_scratch):
    *out_refs, meta_ref = out_and_scratch
    capacity, lanes = values_ref.shape[1:]
    meta_ref[...] = meta_rows(slots_ref, counts_ref, place_ref, lanes)
    pair = lax.div(lax.axis_index("mem"), 2)
    for k, out_ref in enumerate(out_refs):
        rows = pl.ds(2 * lax.bitwise_xor(pair, jnp.int32(k)), 2)
        out_ref[:, pl.ds(0, capacity), :] = values_ref[rows]
        out_ref[:, pl.ds(capacity, META), :] = meta_ref[rows]


def pack(values, slots, counts, groups, paired):
    members, capacity, lanes = values.shape
    place_in_list = pl.pallas_call(
        place_in_list_kernel,
        out_shape=jax.ShapeDtypeStruct(slots.shape, jnp.float32),
        out_specs=vmem_spec(),
        cost_estimate=pl.CostEstimate(flops=2 * 10**9, bytes_accessed=16 * 10**6, transcendentals=0),
        compiler_params=grant(MIB),
        name="place_in_list",
    )()
    if paired:
        kernel, out_shape = pack_pairs_kernel, [lists_shape(2, capacity, lanes)] * (members // 2)
        scratch = [pltpu.VMEM((members, META, lanes), jnp.bfloat16)]
    else:
        kernel, out_shape = pack_groups_kernel, [lists_shape(groups * members, capacity, lanes)]
        scratch = []
    return pl.pallas_call(
        kernel,
        out_shape=out_shape,
        in_specs=[vmem_spec()] * 4,
        out_specs=[vmem_spec()] * len(out_shape),
        scratch_shapes=scratch,
        compiler_params=grant(8 * MIB),
        name="pack",
    )(values, slots, counts, place_in_list)


def digits_of(refs):
    capacity = refs[0].shape[1] - META
    meta = [ref[:, pl.ds(capacity, META), :].astype(jnp.float32) for ref in refs]
    return jnp.concatenate([m[:, 0, :] for m in meta], axis=0), jnp.concatenate([m[:, 1, :] for m in meta], axis=0)


def entries_of(refs):
    capacity, lanes = refs[0].shape[1] - META, refs[0].shape[2]
    return jnp.concatenate([ref[:, pl.ds(0, capacity), :].reshape(-1, lanes) for ref in refs], axis=0)


def as_row(digit, capacity):
    lists, lanes = digit.shape
    per_block = lanes // capacity
    part = lax.broadcasted_iota(jnp.int32, (1, lanes), 1) // capacity
    blocks = []
    for block in range(lists // per_block):
        row = digit[block * per_block : block * per_block + 1]
        for k in range(1, per_block):
            at = block * per_block + k
            row = jnp.where(part == k, digit[at : at + 1], row)
        blocks.append(row)
    return jnp.concatenate(blocks, axis=1)


def as_column(digit, capacity):
    lists, lanes = digit.shape
    shape = (lists, capacity, lanes)
    here = lax.broadcasted_iota(jnp.int32, shape, 2) == lax.broadcasted_iota(jnp.int32, shape, 1)
    picked = jnp.where(here, digit[:, None, :], 0.0).astype(jnp.bfloat16).reshape(lists * capacity, lanes)
    return jnp.dot(picked, jnp.ones((lanes, lanes), jnp.bfloat16), preferred_element_type=jnp.float32)


def keys_of(refs):
    high, low = digits_of(refs)
    return as_row(high * DIGIT + low, refs[0].shape[1] - META)


def answer_some(asking, key, entries):
    capacity, lanes = asking[0].shape[1] - META, entries.shape[1]
    high, low = digits_of(asking)
    column = as_column(high, capacity) * DIGIT + as_column(low, capacity)
    column = jnp.where(column < 0.0, -1.0, column)
    onehot = jnp.concatenate(
        [
            (column == key[:, at : at + lanes]).astype(jnp.float32).astype(jnp.bfloat16)
            for at in range(0, entries.shape[0], lanes)
        ],
        axis=1,
    )
    sums = jnp.dot(onehot, entries, preferred_element_type=jnp.float32)
    count = jnp.dot(onehot, jnp.ones_like(entries), preferred_element_type=jnp.float32)
    mean = sums / jnp.maximum(count, 1.0)
    return mean.astype(jnp.bfloat16).reshape(-1, capacity, lanes)


def answer_kernel(lists_ref, out_ref, key_ref):
    members = out_ref.shape[0]
    step = math.gcd(members, 8)
    key_ref[...] = keys_of([lists_ref])
    first = lax.axis_index("grp") * members

    @pl.loop(0, members, step=step)
    def _(at):
        asking = lists_ref.at[pl.ds(first + at, step)]
        out_ref[pl.ds(at, step)] = answer_some([asking], key_ref[...], entries_of([lists_ref]))


def answer(lists, members):
    senders, rows, lanes = lists.shape
    capacity = rows - META
    entries = senders * capacity
    return pl.pallas_call(
        answer_kernel,
        out_shape=jax.ShapeDtypeStruct((members, capacity, lanes), jnp.bfloat16),
        in_specs=[vmem_spec()],
        out_specs=vmem_spec(),
        scratch_shapes=[pltpu.VMEM((1, entries), jnp.float32)],
        compiler_params=grant(48 * entries * lanes),
        name="answer",
    )(lists)


def pair_answer_kernel(count, *refs):
    in_refs, out_refs = refs[:count], refs[count:]
    for bucket in range(2):
        views = [ref.at[bucket] for ref in in_refs]
        mean = answer_some(views[:1], keys_of(views), entries_of(views))
        for k, out_ref in enumerate(out_refs):
            out_ref[bucket] = mean[k]


def pair_answer(parts):
    pairs, rows, lanes = parts[0].shape[1:]
    shape = jax.ShapeDtypeStruct((2, rows - META, lanes), jnp.bfloat16)
    return pl.pallas_call(
        functools.partial(pair_answer_kernel, len(parts)),
        out_shape=[shape] * pairs,
        in_specs=[vmem_spec()] * len(parts),
        out_specs=[vmem_spec()] * pairs,
        compiler_params=grant(8 * MIB),
        name="pair_answer",
    )(*parts)


def place_kernel(*refs):
    *parts, out_ref, sems = refs
    pair = lax.div(lax.axis_index("mem"), 2)
    copies = []
    for k, part in enumerate(parts):
        rows = pl.ds(2 * lax.bitwise_xor(pair, jnp.int32(k)), 2)
        copies.append(pltpu.make_async_copy(part, out_ref.at[rows], sems.at[k]))
    for copy in copies:
        copy.start()
    for copy in copies:
        copy.wait()


def place(parts):
    two, capacity, lanes = parts[0].shape
    return pl.pallas_call(
        place_kernel,
        out_shape=jax.ShapeDtypeStruct((two * len(parts), capacity, lanes), jnp.bfloat16),
        in_specs=[vmem_spec()] * len(parts),
        out_specs=hbm_spec(),
        scratch_shapes=[pltpu.SemaphoreType.DMA((len(parts),))],
        compiler_params=grant(2 * MIB),
        name="place",
    )(*parts)


def dense_cost(entries, lanes, share=1.0):
    flops = int(2 * BUCKET * entries * lanes * share)
    return pl.CostEstimate(flops=flops, bytes_accessed=int(4 * BUCKET * lanes * share), transcendentals=0)


def dense_kernel(lists_ref, out_ref, key_ref):
    @pl.when(pl.program_id(0) == 0)
    def _():
        key_ref[...] = keys_of([lists_ref])

    tile = out_ref.shape[0]
    wanted = (lax.broadcasted_iota(jnp.int32, (tile, 1), 0) + pl.program_id(0) * tile).astype(jnp.float32)
    onehot = (wanted == key_ref[...]).astype(jnp.float32).astype(jnp.bfloat16)
    entries = entries_of([lists_ref])
    sums = jnp.dot(onehot, entries, preferred_element_type=jnp.float32)
    count = jnp.dot(onehot, jnp.ones_like(entries), preferred_element_type=jnp.float32)
    out_ref[...] = sums / jnp.maximum(count, 1.0)


def dense(lists):
    senders, rows, lanes = lists.shape
    entries = senders * (rows - META)
    tile = math.gcd(BUCKET, 512)
    return pl.pallas_call(
        dense_kernel,
        grid=(BUCKET // tile,),
        out_shape=jax.ShapeDtypeStruct((BUCKET, lanes), jnp.float32),
        in_specs=[vmem_spec()],
        out_specs=pl.BlockSpec((tile, lanes), lambda i: (i, 0)),
        scratch_shapes=[pltpu.VMEM((1, entries), jnp.float32)],
        cost_estimate=dense_cost(entries, lanes),
        name="dense",
    )(lists)


def own_bucket(refs):
    return [ref.at[lax.rem(lax.axis_index("mem"), 2)] for ref in refs]


def dense_prepare_kernel(*refs):
    *in_refs, same_ref, tile_ref, inverse_ref = refs
    views = own_bucket(in_refs)
    capacity, lanes = views[0].shape[1] - META, views[0].shape[2]
    entries = same_ref.shape[1]
    ratio = TILE // DIGIT
    high, low = digits_of(views)
    tile = jnp.floor(high * (1.0 / ratio))
    low_row = as_row(low + DIGIT * (high - ratio * tile), capacity)
    wanted = lax.broadcasted_iota(jnp.int32, (TILE, lanes), 0).astype(jnp.float32)
    for at in range(0, entries, lanes):
        same = (wanted == low_row[:, at : at + lanes]).astype(jnp.float32)
        same_ref[:, at : at + lanes] = same.astype(jnp.bfloat16)
    tile_column = as_column(tile, capacity)
    tile_ref[...] = tile_column.astype(jnp.bfloat16)
    lane = lax.broadcasted_iota(jnp.int32, (entries, lanes), 1).astype(jnp.float32)
    in_tile = (tile_column == lane).astype(jnp.float32).astype(jnp.bfloat16)
    number = jnp.dot(same_ref[...], in_tile, preferred_element_type=jnp.float32)
    inverse_ref[...] = 1.0 / jnp.maximum(number, 1.0)


def dense_tiles_kernel(*refs):
    *in_refs, same_ref, tile_ref, inverse_ref, out_ref, mean_ref, sems = refs
    views = own_bucket(in_refs)
    lanes = views[0].shape[2]
    copies = []
    for pair in range(sems.shape[0]):
        values = entries_of(views)
        tile_of = tile_ref[...]
        zero = jnp.zeros_like(values)
        picked = jnp.concatenate([jnp.where(tile_of == 2 * pair + k, values, zero) for k in range(2)], axis=1)
        sums = jnp.dot(same_ref[...], picked, preferred_element_type=jnp.float32)
        for k in range(2):
            tile = 2 * pair + k
            where = pl.ds(tile * TILE, TILE)
            mean_ref[where, :] = sums[:, k * lanes : (k + 1) * lanes] * inverse_ref[:, tile : tile + 1]
            copy = pltpu.make_async_copy(mean_ref.at[where], out_ref.at[where], sems.at[pair, k])
            copy.start()
            copies.append(copy)
    for copy in copies:
        copy.wait()


def pair_dense(parts):
    _, pairs, rows, _ = parts[0].shape
    entries = len(parts) * pairs * (rows - META)
    prepared = dense_prepare(parts, entries)
    return dense_tiles(parts, prepared)


def dense_prepare(parts, entries):
    lanes = parts[0].shape[3]
    return pl.pallas_call(
        dense_prepare_kernel,
        out_shape=[
            jax.ShapeDtypeStruct((TILE, entries), jnp.bfloat16),
            jax.ShapeDtypeStruct((entries, lanes), jnp.bfloat16),
            jax.ShapeDtypeStruct((TILE, lanes), jnp.float32),
        ],
        in_specs=[vmem_spec()] * len(parts),
        out_specs=[vmem_spec()] * 3,
        cost_estimate=dense_cost(entries, lanes, TILE / BUCKET),
        compiler_params=grant(8 * MIB),
        name="dense_prepare",
    )(*parts)


def dense_tiles(parts, prepared):
    entries, lanes = prepared[1].shape
    return pl.pallas_call(
        dense_tiles_kernel,
        out_shape=jax.ShapeDtypeStruct((BUCKET, lanes), jnp.float32),
        in_specs=[vmem_spec()] * (len(parts) + 3),
        out_specs=hbm_spec(),
        scratch_shapes=[
            pltpu.VMEM((BUCKET, lanes), jnp.float32),
            pltpu.SemaphoreType.DMA((BUCKET // (2 * TILE), 2)),
        ],
        cost_estimate=dense_cost(entries, lanes),
        compiler_params=grant(16 * MIB),
        name="dense_tiles",
    )(*parts, *prepared)


def by_pairs(values, slots, counts, groups):
    members = values.shape[0]
    pairs = members // 2

    def swap(array, axis, size, by):
        return lax.ppermute(array, axis, [(i, i ^ by) for i in range(size)])

    sent = pack(values, slots, counts, groups, True)
    mine = [sent[0]] + [swap(sent[k], "mem", members, 2 * k) for k in range(1, pairs)]
    mine = jnp.stack(mine, axis=1)
    parts = [mine] + [swap(mine, "grp", groups, k) for k in range(1, groups)]
    parts = parts + [swap(part, "mem", members, 1) for part in parts]
    answers = pair_answer(parts)
    averaged = pair_dense(parts)
    back = [answers[0]] + [swap(answers[k], "mem", members, 2 * k) for k in range(1, pairs)]
    return averaged, place(back)


def by_all(values, slots, counts, groups):
    members = values.shape[0]
    (lists,) = pack(values, slots, counts, groups, False)
    got = lax.all_to_all(lists, ("grp", "mem"), split_axis=0, concat_axis=0, tiled=True)
    back = answer(got, members)
    returned = lax.all_to_all(back, "mem", split_axis=0, concat_axis=0, tiled=True)
    return dense(got), returned


def per_device(groups, values, slots, counts):
    members, capacity, lanes = values.shape[1:]
    entries = groups * members * capacity
    few = members in (2, 4, 8) and groups in (1, 2, 4, 8) and entries <= 2048
    tiles = BUCKET % (2 * TILE) == 0 and BUCKET // TILE <= lanes
    move = by_pairs if few and tiles else by_all
    averaged, returned = move(values[0], slots[0], counts, groups)
    return (averaged, returned[None])


def one_step(groups, values, slots, counts):
    return per_device(groups, values, slots, counts)


def solution(mesh):
    return jax.shard_map(
        functools.partial(one_step, mesh.shape["grp"]),
        mesh=mesh,
        in_specs=(
            P(("grp", "mem"), None, None, None),
            P(("grp", "mem"), None, None),
            P(("grp", "mem"), None),
        ),
        out_specs=(P("mem", None), P(("grp", "mem"), None, None, None)),
        check_vma=False,
    )
```

```python
import functools
import math

import jax
import jax.numpy as jnp
from jax import lax
from jax.experimental import pallas as pl
from jax.experimental.pallas import tpu as pltpu
from jax.sharding import PartitionSpec as P


BUCKET = 7168
DIGIT = 256
TILE = 512
META = 8
MIB = 2**20


def vmem_spec():
    return pl.BlockSpec(memory_space=pltpu.VMEM)


def hbm_spec():
    return pl.BlockSpec(memory_space=pltpu.HBM)


def grant(size):
    return pltpu.CompilerParams(vmem_limit_bytes=size)


def lists_shape(count, capacity, lanes):
    return jax.ShapeDtypeStruct((count, capacity + META, lanes), jnp.bfloat16)


def place_in_list_kernel(out_ref):
    out_ref[...] = lax.broadcasted_iota(jnp.int32, out_ref.shape, 1).astype(jnp.float32)


def meta_rows(slots_ref, counts_ref, place_ref, lanes):
    members, capacity = slots_ref.shape
    shape = (members, members)
    diagonal = lax.broadcasted_iota(jnp.int32, shape, 0) == lax.broadcasted_iota(jnp.int32, shape, 1)
    count = jnp.sum(jnp.where(diagonal, counts_ref[...].astype(jnp.float32), 0.0), axis=1, keepdims=True)
    slot = slots_ref[...]
    live = place_ref[...] < count
    high = jnp.where(live, (slot // DIGIT).astype(jnp.float32), -1.0)
    low = jnp.where(live, (slot % DIGIT).astype(jnp.float32), 0.0)
    repeats = lanes // capacity
    high = jnp.concatenate([high] * repeats, axis=1)
    low = jnp.concatenate([low] * repeats, axis=1)
    row = lax.broadcasted_iota(jnp.int32, (members, META, lanes), 1)
    return jnp.where(row == 0, high[:, None, :], low[:, None, :]).astype(jnp.bfloat16)


def pack_groups_kernel(values_ref, slots_ref, counts_ref, place_ref, out_ref):
    members, capacity, lanes = values_ref.shape
    meta = meta_rows(slots_ref, counts_ref, place_ref, lanes)
    for group in range(out_ref.shape[0] // members):
        rows = pl.ds(group * members, members)
        out_ref[rows, pl.ds(0, capacity), :] = values_ref[...]
        out_ref[rows, pl.ds(capacity, META), :] = meta


def pack_pairs_kernel(values_ref, slots_ref, counts_ref, place_ref, *out_and_scratch):
    *out_refs, meta_ref = out_and_scratch
    capacity, lanes = values_ref.shape[1:]
    meta_ref[...] = meta_rows(slots_ref, counts_ref, place_ref, lanes)
    pair = lax.div(lax.axis_index("mem"), 2)
    for k, out_ref in enumerate(out_refs):
        rows = pl.ds(2 * lax.bitwise_xor(pair, jnp.int32(k)), 2)
        out_ref[:, pl.ds(0, capacity), :] = values_ref[rows]
        out_ref[:, pl.ds(capacity, META), :] = meta_ref[rows]


def pack(values, slots, counts, groups, paired):
    members, capacity, lanes = values.shape
    place_in_list = pl.pallas_call(
        place_in_list_kernel,
        out_shape=jax.ShapeDtypeStruct(slots.shape, jnp.float32),
        out_specs=vmem_spec(),
        cost_estimate=pl.CostEstimate(flops=2 * 10**9, bytes_accessed=16 * 10**6, transcendentals=0),
        compiler_params=grant(MIB),
        name="place_in_list",
    )()
    if paired:
        kernel, out_shape = pack_pairs_kernel, [lists_shape(2, capacity, lanes)] * (members // 2)
        scratch = [pltpu.VMEM((members, META, lanes), jnp.bfloat16)]
    else:
        kernel, out_shape = pack_groups_kernel, [lists_shape(groups * members, capacity, lanes)]
        scratch = []
    return pl.pallas_call(
        kernel,
        out_shape=out_shape,
        in_specs=[vmem_spec()] * 4,
        out_specs=[vmem_spec()] * len(out_shape),
        scratch_shapes=scratch,
        compiler_params=grant(8 * MIB),
        name="pack",
    )(values, slots, counts, place_in_list)


def digits_of(refs):
    capacity = refs[0].shape[1] - META
    meta = [ref[:, pl.ds(capacity, META), :].astype(jnp.float32) for ref in refs]
    return jnp.concatenate([m[:, 0, :] for m in meta], axis=0), jnp.concatenate([m[:, 1, :] for m in meta], axis=0)


def entries_of(refs):
    capacity, lanes = refs[0].shape[1] - META, refs[0].shape[2]
    return jnp.concatenate([ref[:, pl.ds(0, capacity), :].reshape(-1, lanes) for ref in refs], axis=0)


def as_row(digit, capacity):
    lists, lanes = digit.shape
    per_block = lanes // capacity
    part = lax.broadcasted_iota(jnp.int32, (1, lanes), 1) // capacity
    blocks = []
    for block in range(lists // per_block):
        row = digit[block * per_block : block * per_block + 1]
        for k in range(1, per_block):
            at = block * per_block + k
            row = jnp.where(part == k, digit[at : at + 1], row)
        blocks.append(row)
    return jnp.concatenate(blocks, axis=1)


def as_column(digit, capacity):
    lists, lanes = digit.shape
    shape = (lists, capacity, lanes)
    here = lax.broadcasted_iota(jnp.int32, shape, 2) == lax.broadcasted_iota(jnp.int32, shape, 1)
    picked = jnp.where(here, digit[:, None, :], 0.0).astype(jnp.bfloat16).reshape(lists * capacity, lanes)
    return jnp.dot(picked, jnp.ones((lanes, lanes), jnp.bfloat16), preferred_element_type=jnp.float32)


def keys_of(refs):
    high, low = digits_of(refs)
    return as_row(high * DIGIT + low, refs[0].shape[1] - META)


def asked_column(asking):
    capacity = asking[0].shape[1] - META
    high, low = digits_of(asking)
    column = as_column(high, capacity) * DIGIT + as_column(low, capacity)
    return jnp.where(column < 0.0, -1.0, column)


def matching_sums(column, key, entries):
    lanes = entries.shape[1]
    onehot = jnp.concatenate(
        [
            (column == key[:, at : at + lanes]).astype(jnp.float32).astype(jnp.bfloat16)
            for at in range(0, entries.shape[0], lanes)
        ],
        axis=1,
    )
    sums = jnp.dot(onehot, entries, preferred_element_type=jnp.float32)
    return sums, jnp.dot(onehot, jnp.ones_like(entries), preferred_element_type=jnp.float32)


def answer_kernel(lists_ref, out_ref, key_ref):
    members = out_ref.shape[0]
    step = math.gcd(members, 8)
    key_ref[...] = keys_of([lists_ref])
    first = lax.axis_index("grp") * members

    @pl.loop(0, members, step=step)
    def _(at):
        asking = lists_ref.at[pl.ds(first + at, step)]
        sums, count = matching_sums(asked_column([asking]), key_ref[...], entries_of([lists_ref]))
        mean = sums / jnp.maximum(count, 1.0)
        out_ref[pl.ds(at, step)] = mean.astype(jnp.bfloat16).reshape(step, *out_ref.shape[1:])


def answer(lists, members):
    senders, rows, lanes = lists.shape
    capacity = rows - META
    entries = senders * capacity
    return pl.pallas_call(
        answer_kernel,
        out_shape=jax.ShapeDtypeStruct((members, capacity, lanes), jnp.bfloat16),
        in_specs=[vmem_spec()],
        out_specs=vmem_spec(),
        scratch_shapes=[pltpu.VMEM((1, entries), jnp.float32)],
        compiler_params=grant(48 * entries * lanes),
        name="answer",
    )(lists)


def begin_answer_kernel(*refs):
    *in_refs, column_ref, sums_ref, count_ref = refs
    for bucket in range(2):
        views = [ref.at[bucket] for ref in in_refs]
        column = asked_column(views[:1])
        sums, count = matching_sums(column, keys_of(views), entries_of(views))
        column_ref[bucket] = column
        sums_ref[bucket] = sums
        count_ref[bucket] = count


def finish_answer_kernel(count, *refs):
    in_refs, (column_ref, sums_ref, count_ref), out_refs = refs[:count], refs[count : count + 3], refs[count + 3 :]
    for bucket in range(2):
        views = [ref.at[bucket] for ref in in_refs]
        sums, number = matching_sums(column_ref[bucket], keys_of(views), entries_of(views))
        mean = (sums_ref[bucket] + sums) / jnp.maximum(count_ref[bucket] + number, 1.0)
        mean = mean.astype(jnp.bfloat16).reshape(len(out_refs), *out_refs[0].shape[1:])
        for k, out_ref in enumerate(out_refs):
            out_ref[bucket] = mean[k]


def begin_answer(parts):
    pairs, rows, lanes = parts[0].shape[1:]
    partial = jax.ShapeDtypeStruct((2, pairs * (rows - META), lanes), jnp.float32)
    return pl.pallas_call(
        begin_answer_kernel,
        out_shape=[partial] * 3,
        in_specs=[vmem_spec()] * len(parts),
        out_specs=[vmem_spec()] * 3,
        compiler_params=grant(8 * MIB),
        name="begin_answer",
    )(*parts)


def finish_answer(parts, begun):
    pairs, rows, lanes = parts[0].shape[1:]
    shape = jax.ShapeDtypeStruct((2, rows - META, lanes), jnp.bfloat16)
    return pl.pallas_call(
        functools.partial(finish_answer_kernel, len(parts)),
        out_shape=[shape] * pairs,
        in_specs=[vmem_spec()] * (len(parts) + 3),
        out_specs=[vmem_spec()] * pairs,
        compiler_params=grant(8 * MIB),
        name="finish_answer",
    )(*parts, *begun)


def place_kernel(*refs):
    *parts, out_ref, sems = refs
    pair = lax.div(lax.axis_index("mem"), 2)
    copies = []
    for k, part in enumerate(parts):
        rows = pl.ds(2 * lax.bitwise_xor(pair, jnp.int32(k)), 2)
        copies.append(pltpu.make_async_copy(part, out_ref.at[rows], sems.at[k]))
    for copy in copies:
        copy.start()
    for copy in copies:
        copy.wait()


def place(parts):
    two, capacity, lanes = parts[0].shape
    return pl.pallas_call(
        place_kernel,
        out_shape=jax.ShapeDtypeStruct((two * len(parts), capacity, lanes), jnp.bfloat16),
        in_specs=[vmem_spec()] * len(parts),
        out_specs=hbm_spec(),
        scratch_shapes=[pltpu.SemaphoreType.DMA((len(parts),))],
        compiler_params=grant(2 * MIB),
        name="place",
    )(*parts)


def dense_cost(entries, lanes, share=1.0):
    flops = int(2 * BUCKET * entries * lanes * share)
    return pl.CostEstimate(flops=flops, bytes_accessed=int(4 * BUCKET * lanes * share), transcendentals=0)


def dense_kernel(lists_ref, out_ref, key_ref):
    @pl.when(pl.program_id(0) == 0)
    def _():
        key_ref[...] = keys_of([lists_ref])

    tile = out_ref.shape[0]
    wanted = (lax.broadcasted_iota(jnp.int32, (tile, 1), 0) + pl.program_id(0) * tile).astype(jnp.float32)
    onehot = (wanted == key_ref[...]).astype(jnp.float32).astype(jnp.bfloat16)
    entries = entries_of([lists_ref])
    sums = jnp.dot(onehot, entries, preferred_element_type=jnp.float32)
    count = jnp.dot(onehot, jnp.ones_like(entries), preferred_element_type=jnp.float32)
    out_ref[...] = sums / jnp.maximum(count, 1.0)


def dense(lists):
    senders, rows, lanes = lists.shape
    entries = senders * (rows - META)
    tile = math.gcd(BUCKET, 512)
    return pl.pallas_call(
        dense_kernel,
        grid=(BUCKET // tile,),
        out_shape=jax.ShapeDtypeStruct((BUCKET, lanes), jnp.float32),
        in_specs=[vmem_spec()],
        out_specs=pl.BlockSpec((tile, lanes), lambda i: (i, 0)),
        scratch_shapes=[pltpu.VMEM((1, entries), jnp.float32)],
        cost_estimate=dense_cost(entries, lanes),
        name="dense",
    )(lists)


def own_bucket(refs):
    return [ref.at[lax.rem(lax.axis_index("mem"), 2)] for ref in refs]


def dense_prepare_kernel(*refs):
    *in_refs, same_ref, tile_ref, number_ref = refs
    views = own_bucket(in_refs)
    capacity, lanes = views[0].shape[1] - META, views[0].shape[2]
    entries = same_ref.shape[1]
    ratio = TILE // DIGIT
    high, low = digits_of(views)
    tile = jnp.floor(high * (1.0 / ratio))
    low_row = as_row(low + DIGIT * (high - ratio * tile), capacity)
    wanted = lax.broadcasted_iota(jnp.int32, (TILE, lanes), 0).astype(jnp.float32)
    for at in range(0, entries, lanes):
        same = (wanted == low_row[:, at : at + lanes]).astype(jnp.float32)
        same_ref[:, at : at + lanes] = same.astype(jnp.bfloat16)
    tile_column = as_column(tile, capacity)
    tile_ref[...] = tile_column.astype(jnp.bfloat16)
    lane = lax.broadcasted_iota(jnp.int32, (entries, lanes), 1).astype(jnp.float32)
    in_tile = (tile_column == lane).astype(jnp.float32).astype(jnp.bfloat16)
    number_ref[...] = jnp.dot(same_ref[...], in_tile, preferred_element_type=jnp.float32)


def dense_prepare(parts):
    pairs, rows, lanes = parts[0].shape[1:]
    entries = len(parts) * pairs * (rows - META)
    return pl.pallas_call(
        dense_prepare_kernel,
        out_shape=[
            jax.ShapeDtypeStruct((TILE, entries), jnp.bfloat16),
            jax.ShapeDtypeStruct((entries, lanes), jnp.bfloat16),
            jax.ShapeDtypeStruct((TILE, lanes), jnp.float32),
        ],
        in_specs=[vmem_spec()] * len(parts),
        out_specs=[vmem_spec()] * 3,
        compiler_params=grant(8 * MIB),
        name="dense_prepare",
    )(*parts)


def dense_tiles_kernel(count, *refs):
    in_refs, prepared = refs[:count], refs[count : count + 6]
    out_ref, mean_ref, inverse_ref, sems = refs[count + 6 :]
    views = own_bucket(in_refs)
    lanes = views[0].shape[2]
    inverse_ref[...] = 1.0 / jnp.maximum(prepared[2][...] + prepared[5][...], 1.0)
    copies = []
    for pair in range(sems.shape[0]):
        values = entries_of(views)
        tile_of = jnp.concatenate([prepared[1][...], prepared[4][...]], axis=0)
        same = jnp.concatenate([prepared[0][...], prepared[3][...]], axis=1)
        zero = jnp.zeros_like(values)
        picked = jnp.concatenate([jnp.where(tile_of == 2 * pair + k, values, zero) for k in range(2)], axis=1)
        sums = jnp.dot(same, picked, preferred_element_type=jnp.float32)
        for k in range(2):
            tile = 2 * pair + k
            where = pl.ds(tile * TILE, TILE)
            mean_ref[where, :] = sums[:, k * lanes : (k + 1) * lanes] * inverse_ref[:, tile : tile + 1]
            copy = pltpu.make_async_copy(mean_ref.at[where], out_ref.at[where], sems.at[pair, k])
            copy.start()
            copies.append(copy)
    for copy in copies:
        copy.wait()


def dense_tiles(parts, prepared):
    pairs, rows, lanes = parts[0].shape[1:]
    entries = len(parts) * pairs * (rows - META)
    return pl.pallas_call(
        functools.partial(dense_tiles_kernel, len(parts)),
        out_shape=jax.ShapeDtypeStruct((BUCKET, lanes), jnp.float32),
        in_specs=[vmem_spec()] * (len(parts) + len(prepared)),
        out_specs=hbm_spec(),
        scratch_shapes=[
            pltpu.VMEM((BUCKET, lanes), jnp.float32),
            pltpu.VMEM((TILE, lanes), jnp.float32),
            pltpu.SemaphoreType.DMA((BUCKET // (2 * TILE), 2)),
        ],
        cost_estimate=dense_cost(entries, lanes),
        compiler_params=grant(16 * MIB),
        name="dense_tiles",
    )(*parts, *prepared)


def by_pairs(values, slots, counts, groups):
    members = values.shape[0]
    pairs = members // 2

    def swap(array, axis, size, by):
        return lax.ppermute(array, axis, [(i, i ^ by) for i in range(size)])

    sent = pack(values, slots, counts, groups, True)
    mine = [sent[0]] + [swap(sent[k], "mem", members, 2 * k) for k in range(1, pairs)]
    mine = jnp.stack(mine, axis=1)
    same = [mine] + [swap(mine, "grp", groups, k) for k in range(1, groups)]
    other = [swap(part, "mem", members, 1) for part in same]
    begun = begin_answer(same)
    prepared = dense_prepare(same)
    answers = finish_answer(other, begun)
    prepared += dense_prepare(other)
    averaged = dense_tiles(same + other, prepared)
    back = [answers[0]] + [swap(answers[k], "mem", members, 2 * k) for k in range(1, pairs)]
    return averaged, place(back)


def by_all(values, slots, counts, groups):
    members = values.shape[0]
    (lists,) = pack(values, slots, counts, groups, False)
    got = lax.all_to_all(lists, ("grp", "mem"), split_axis=0, concat_axis=0, tiled=True)
    back = answer(got, members)
    returned = lax.all_to_all(back, "mem", split_axis=0, concat_axis=0, tiled=True)
    return dense(got), returned


def per_device(groups, values, slots, counts):
    members, capacity, lanes = values.shape[1:]
    entries = groups * members * capacity
    few = members in (2, 4, 8) and groups in (1, 2, 4, 8) and entries <= 2048
    tiles = BUCKET % (2 * TILE) == 0 and BUCKET // TILE <= lanes
    move = by_pairs if few and tiles else by_all
    averaged, returned = move(values[0], slots[0], counts, groups)
    return (averaged, returned[None])


def one_step(groups, values, slots, counts):
    return per_device(groups, values, slots, counts)


def solution(mesh):
    return jax.shard_map(
        functools.partial(one_step, mesh.shape["grp"]),
        mesh=mesh,
        in_specs=(
            P(("grp", "mem"), None, None, None),
            P(("grp", "mem"), None, None),
            P(("grp", "mem"), None),
        ),
        out_specs=(P("mem", None), P(("grp", "mem"), None, None, None)),
        check_vma=False,
    )
```

```python
import functools
import math

import jax
import jax.numpy as jnp
from jax import lax
from jax.experimental import pallas as pl
from jax.experimental.pallas import tpu as pltpu
from jax.sharding import PartitionSpec as P


BUCKET = 7168
DIGIT = 256
TILE = 512
META = 8
MIB = 2**20


def vmem_spec():
    return pl.BlockSpec(memory_space=pltpu.VMEM)


def hbm_spec():
    return pl.BlockSpec(memory_space=pltpu.HBM)


def grant(size):
    return pltpu.CompilerParams(vmem_limit_bytes=size)


def lists_shape(count, capacity, lanes):
    return jax.ShapeDtypeStruct((count, capacity + META, lanes), jnp.bfloat16)


def place_in_list_kernel(out_ref):
    out_ref[...] = lax.broadcasted_iota(jnp.int32, out_ref.shape, 1).astype(jnp.float32)


def meta_rows(slots_ref, counts_ref, place_ref, lanes):
    members, capacity = slots_ref.shape
    shape = (members, members)
    diagonal = lax.broadcasted_iota(jnp.int32, shape, 0) == lax.broadcasted_iota(jnp.int32, shape, 1)
    count = jnp.sum(jnp.where(diagonal, counts_ref[...].astype(jnp.float32), 0.0), axis=1, keepdims=True)
    slot = slots_ref[...]
    live = place_ref[...] < count
    high = jnp.where(live, (slot // DIGIT).astype(jnp.float32), -1.0)
    low = jnp.where(live, (slot % DIGIT).astype(jnp.float32), 0.0)
    repeats = lanes // capacity
    high = jnp.concatenate([high] * repeats, axis=1)
    low = jnp.concatenate([low] * repeats, axis=1)
    row = lax.broadcasted_iota(jnp.int32, (members, META, lanes), 1)
    return jnp.where(row == 0, high[:, None, :], low[:, None, :]).astype(jnp.bfloat16)


def pack_groups_kernel(values_ref, slots_ref, counts_ref, place_ref, out_ref):
    members, capacity, lanes = values_ref.shape
    meta = meta_rows(slots_ref, counts_ref, place_ref, lanes)
    for group in range(out_ref.shape[0] // members):
        rows = pl.ds(group * members, members)
        out_ref[rows, pl.ds(0, capacity), :] = values_ref[...]
        out_ref[rows, pl.ds(capacity, META), :] = meta


def pack_pairs_kernel(values_ref, slots_ref, counts_ref, place_ref, *out_and_scratch):
    *out_refs, meta_ref = out_and_scratch
    capacity, lanes = values_ref.shape[1:]
    meta_ref[...] = meta_rows(slots_ref, counts_ref, place_ref, lanes)
    pair = lax.div(lax.axis_index("mem"), 2)
    for k, out_ref in enumerate(out_refs):
        rows = pl.ds(2 * lax.bitwise_xor(pair, jnp.int32(k)), 2)
        out_ref[:, pl.ds(0, capacity), :] = values_ref[rows]
        out_ref[:, pl.ds(capacity, META), :] = meta_ref[rows]


def pack(values, slots, counts, groups, paired):
    members, capacity, lanes = values.shape
    place_in_list = pl.pallas_call(
        place_in_list_kernel,
        out_shape=jax.ShapeDtypeStruct(slots.shape, jnp.float32),
        out_specs=vmem_spec(),
        cost_estimate=pl.CostEstimate(flops=2 * 10**9, bytes_accessed=16 * 10**6, transcendentals=0),
        compiler_params=grant(MIB),
        name="place_in_list",
    )()
    if paired:
        kernel, out_shape = pack_pairs_kernel, [lists_shape(2, capacity, lanes)] * (members // 2)
        scratch = [pltpu.VMEM((members, META, lanes), jnp.bfloat16)]
    else:
        kernel, out_shape = pack_groups_kernel, [lists_shape(groups * members, capacity, lanes)]
        scratch = []
    return pl.pallas_call(
        kernel,
        out_shape=out_shape,
        in_specs=[vmem_spec()] * 4,
        out_specs=[vmem_spec()] * len(out_shape),
        scratch_shapes=scratch,
        compiler_params=grant(8 * MIB),
        name="pack",
    )(values, slots, counts, place_in_list)


def digits_of(refs):
    capacity = refs[0].shape[1] - META
    meta = [ref[:, pl.ds(capacity, META), :].astype(jnp.float32) for ref in refs]
    return jnp.concatenate([m[:, 0, :] for m in meta], axis=0), jnp.concatenate([m[:, 1, :] for m in meta], axis=0)


def entries_of(refs):
    capacity, lanes = refs[0].shape[1] - META, refs[0].shape[2]
    return jnp.concatenate([ref[:, pl.ds(0, capacity), :].reshape(-1, lanes) for ref in refs], axis=0)


def as_row(digit, capacity):
    lists, lanes = digit.shape
    per_block = lanes // capacity
    part = lax.broadcasted_iota(jnp.int32, (1, lanes), 1) // capacity
    blocks = []
    for block in range(lists // per_block):
        row = digit[block * per_block : block * per_block + 1]
        for k in range(1, per_block):
            at = block * per_block + k
            row = jnp.where(part == k, digit[at : at + 1], row)
        blocks.append(row)
    return jnp.concatenate(blocks, axis=1)


def as_column(digit, capacity):
    lists, lanes = digit.shape
    shape = (lists, capacity, lanes)
    here = lax.broadcasted_iota(jnp.int32, shape, 2) == lax.broadcasted_iota(jnp.int32, shape, 1)
    picked = jnp.where(here, digit[:, None, :], 0.0).astype(jnp.bfloat16).reshape(lists * capacity, lanes)
    return jnp.dot(picked, jnp.ones((lanes, lanes), jnp.bfloat16), preferred_element_type=jnp.float32)


def keys_of(refs):
    high, low = digits_of(refs)
    return as_row(high * DIGIT + low, refs[0].shape[1] - META)


def asked_column(asking):
    capacity = asking[0].shape[1] - META
    high, low = digits_of(asking)
    column = as_column(high, capacity) * DIGIT + as_column(low, capacity)
    return jnp.where(column < 0.0, -1.0, column)


def matching_sums(column, key, entries):
    lanes = entries.shape[1]
    onehot = jnp.concatenate(
        [
            (column == key[:, at : at + lanes]).astype(jnp.float32).astype(jnp.bfloat16)
            for at in range(0, entries.shape[0], lanes)
        ],
        axis=1,
    )
    sums = jnp.dot(onehot, entries, preferred_element_type=jnp.float32)
    return sums, jnp.dot(onehot, jnp.ones_like(entries), preferred_element_type=jnp.float32)


def answer_kernel(lists_ref, out_ref, key_ref):
    members = out_ref.shape[0]
    step = math.gcd(members, 8)
    key_ref[...] = keys_of([lists_ref])
    first = lax.axis_index("grp") * members

    @pl.loop(0, members, step=step)
    def _(at):
        asking = lists_ref.at[pl.ds(first + at, step)]
        sums, count = matching_sums(asked_column([asking]), key_ref[...], entries_of([lists_ref]))
        mean = sums / jnp.maximum(count, 1.0)
        out_ref[pl.ds(at, step)] = mean.astype(jnp.bfloat16).reshape(step, *out_ref.shape[1:])


def answer(lists, members):
    senders, rows, lanes = lists.shape
    capacity = rows - META
    entries = senders * capacity
    return pl.pallas_call(
        answer_kernel,
        out_shape=jax.ShapeDtypeStruct((members, capacity, lanes), jnp.bfloat16),
        in_specs=[vmem_spec()],
        out_specs=vmem_spec(),
        scratch_shapes=[pltpu.VMEM((1, entries), jnp.float32)],
        compiler_params=grant(48 * entries * lanes),
        name="answer",
    )(lists)


def partial_answer(refs, bucket, column_ref):
    views = [ref.at[bucket] for ref in refs]
    return matching_sums(column_ref[bucket], keys_of(views), entries_of(views))


def begin_answer_kernel(*refs):
    *in_refs, column_ref, sums_ref, count_ref = refs
    for bucket in range(2):
        column_ref[bucket] = asked_column([in_refs[0].at[bucket]])
        sums_ref[bucket], count_ref[bucket] = partial_answer(in_refs, bucket, column_ref)


def more_answer_kernel(*refs):
    *in_refs, column_ref, sums_ref, count_ref, new_sums_ref, new_count_ref = refs
    for bucket in range(2):
        sums, number = partial_answer(in_refs, bucket, column_ref)
        new_sums_ref[bucket] = sums_ref[bucket] + sums
        new_count_ref[bucket] = count_ref[bucket] + number


def finish_answer_kernel(count, *refs):
    in_refs, (column_ref, sums_ref, count_ref), out_refs = refs[:count], refs[count : count + 3], refs[count + 3 :]
    for bucket in range(2):
        sums, number = partial_answer(in_refs, bucket, column_ref)
        mean = (sums_ref[bucket] + sums) / jnp.maximum(count_ref[bucket] + number, 1.0)
        mean = mean.astype(jnp.bfloat16).reshape(len(out_refs), *out_refs[0].shape[1:])
        for k, out_ref in enumerate(out_refs):
            out_ref[bucket] = mean[k]


def run_answer(kernel, out_shape, operands):
    return pl.pallas_call(
        kernel,
        out_shape=out_shape,
        in_specs=[vmem_spec()] * len(operands),
        out_specs=[vmem_spec()] * len(out_shape),
        compiler_params=grant(8 * MIB),
    )(*operands)


def begin_answer(parts):
    pairs, rows, lanes = parts[0].shape[1:]
    partial = jax.ShapeDtypeStruct((2, pairs * (rows - META), lanes), jnp.float32)
    return run_answer(begin_answer_kernel, [partial] * 3, parts)


def more_answer(parts, begun):
    partial = jax.ShapeDtypeStruct(begun[0].shape, jnp.float32)
    return [begun[0], *run_answer(more_answer_kernel, [partial] * 2, [*parts, *begun])]


def finish_answer(parts, begun):
    pairs, rows, lanes = parts[0].shape[1:]
    shape = jax.ShapeDtypeStruct((2, rows - META, lanes), jnp.bfloat16)
    kernel = functools.partial(finish_answer_kernel, len(parts))
    return run_answer(kernel, [shape] * pairs, [*parts, *begun])


def place_kernel(*refs):
    *parts, out_ref, sems = refs
    pair = lax.div(lax.axis_index("mem"), 2)
    copies = []
    for k, part in enumerate(parts):
        rows = pl.ds(2 * lax.bitwise_xor(pair, jnp.int32(k)), 2)
        copies.append(pltpu.make_async_copy(part, out_ref.at[rows], sems.at[k]))
    for copy in copies:
        copy.start()
    for copy in copies:
        copy.wait()


def place(parts):
    two, capacity, lanes = parts[0].shape
    return pl.pallas_call(
        place_kernel,
        out_shape=jax.ShapeDtypeStruct((two * len(parts), capacity, lanes), jnp.bfloat16),
        in_specs=[vmem_spec()] * len(parts),
        out_specs=hbm_spec(),
        scratch_shapes=[pltpu.SemaphoreType.DMA((len(parts),))],
        compiler_params=grant(2 * MIB),
        name="place",
    )(*parts)


def dense_cost(entries, lanes, share=1.0):
    flops = int(2 * BUCKET * entries * lanes * share)
    return pl.CostEstimate(flops=flops, bytes_accessed=int(4 * BUCKET * lanes * share), transcendentals=0)


def dense_kernel(lists_ref, out_ref, key_ref):
    @pl.when(pl.program_id(0) == 0)
    def _():
        key_ref[...] = keys_of([lists_ref])

    tile = out_ref.shape[0]
    wanted = (lax.broadcasted_iota(jnp.int32, (tile, 1), 0) + pl.program_id(0) * tile).astype(jnp.float32)
    onehot = (wanted == key_ref[...]).astype(jnp.float32).astype(jnp.bfloat16)
    entries = entries_of([lists_ref])
    sums = jnp.dot(onehot, entries, preferred_element_type=jnp.float32)
    count = jnp.dot(onehot, jnp.ones_like(entries), preferred_element_type=jnp.float32)
    out_ref[...] = sums / jnp.maximum(count, 1.0)


def dense(lists):
    senders, rows, lanes = lists.shape
    entries = senders * (rows - META)
    tile = math.gcd(BUCKET, 512)
    return pl.pallas_call(
        dense_kernel,
        grid=(BUCKET // tile,),
        out_shape=jax.ShapeDtypeStruct((BUCKET, lanes), jnp.float32),
        in_specs=[vmem_spec()],
        out_specs=pl.BlockSpec((tile, lanes), lambda i: (i, 0)),
        scratch_shapes=[pltpu.VMEM((1, entries), jnp.float32)],
        cost_estimate=dense_cost(entries, lanes),
        name="dense",
    )(lists)


def own_bucket(refs):
    return [ref.at[lax.rem(lax.axis_index("mem"), 2)] for ref in refs]


def prepare_tiles(views, same_ref, tile_ref, number_ref):
    capacity, lanes = views[0].shape[1] - META, views[0].shape[2]
    entries = same_ref.shape[1]
    ratio = TILE // DIGIT
    high, low = digits_of(views)
    tile = jnp.floor(high * (1.0 / ratio))
    low_row = as_row(low + DIGIT * (high - ratio * tile), capacity)
    wanted = lax.broadcasted_iota(jnp.int32, (TILE, lanes), 0).astype(jnp.float32)
    for at in range(0, entries, lanes):
        same = (wanted == low_row[:, at : at + lanes]).astype(jnp.float32)
        same_ref[:, at : at + lanes] = same.astype(jnp.bfloat16)
    tile_column = as_column(tile, capacity)
    tile_ref[...] = tile_column.astype(jnp.bfloat16)
    lane = lax.broadcasted_iota(jnp.int32, (entries, lanes), 1).astype(jnp.float32)
    in_tile = (tile_column == lane).astype(jnp.float32).astype(jnp.bfloat16)
    number_ref[...] = jnp.dot(same_ref[...], in_tile, preferred_element_type=jnp.float32)


def dense_prepare_kernel(*refs):
    *in_refs, same_ref, tile_ref, number_ref = refs
    prepare_tiles(own_bucket(in_refs), same_ref, tile_ref, number_ref)


def dense_prepare(parts):
    pairs, rows, lanes = parts[0].shape[1:]
    entries = len(parts) * pairs * (rows - META)
    return pl.pallas_call(
        dense_prepare_kernel,
        out_shape=[
            jax.ShapeDtypeStruct((TILE, entries), jnp.bfloat16),
            jax.ShapeDtypeStruct((entries, lanes), jnp.bfloat16),
            jax.ShapeDtypeStruct((TILE, lanes), jnp.float32),
        ],
        in_specs=[vmem_spec()] * len(parts),
        out_specs=[vmem_spec()] * 3,
        compiler_params=grant(8 * MIB),
        name="dense_prepare",
    )(*parts)


def pair_sums(pair, views, same_refs, tile_refs):
    values = entries_of(views)
    tile_of = jnp.concatenate([ref[...] for ref in tile_refs], axis=0)
    same = jnp.concatenate([ref[...] for ref in same_refs], axis=1)
    zero = jnp.zeros_like(values)
    picked = jnp.concatenate([jnp.where(tile_of == 2 * pair + k, values, zero) for k in range(2)], axis=1)
    return jnp.dot(same, picked, preferred_element_type=jnp.float32)


def begin_tiles_kernel(*refs):
    *in_refs, same_ref, tile_ref, out_ref = refs
    views = own_bucket(in_refs)
    lanes = out_ref.shape[1]
    for pair in range(BUCKET // (2 * TILE)):
        sums = pair_sums(pair, views, [same_ref], [tile_ref])
        for k in range(2):
            out_ref[pl.ds((2 * pair + k) * TILE, TILE), :] = sums[:, k * lanes : (k + 1) * lanes]


def begin_tiles(parts, prepared):
    lanes = parts[0].shape[3]
    return pl.pallas_call(
        begin_tiles_kernel,
        out_shape=jax.ShapeDtypeStruct((BUCKET, lanes), jnp.float32),
        in_specs=[vmem_spec()] * (len(parts) + 2),
        out_specs=vmem_spec(),
        compiler_params=grant(8 * MIB),
        name="begin_tiles",
    )(*parts, *prepared[:2])


def finish_tiles_kernel(count, *refs):
    same_parts, other_parts = refs[:count], refs[count : 2 * count]
    begun_ref, number_ref, *middle = refs[2 * count : 2 * count + 5]
    out_ref, mean_ref, inverse_ref, same_ref, tile_ref, last_ref, sems = refs[2 * count + 5 :]
    prepare_tiles(own_bucket(other_parts), same_ref, tile_ref, last_ref)
    views = own_bucket(same_parts + other_parts)
    lanes = views[0].shape[2]
    inverse_ref[...] = 1.0 / jnp.maximum(number_ref[...] + middle[2][...] + last_ref[...], 1.0)
    copies = []
    for pair in range(sems.shape[0]):
        sums = pair_sums(pair, views, [middle[0], same_ref], [middle[1], tile_ref])
        for k in range(2):
            tile = 2 * pair + k
            where = pl.ds(tile * TILE, TILE)
            total = begun_ref[where, :] + sums[:, k * lanes : (k + 1) * lanes]
            mean_ref[where, :] = total * inverse_ref[:, tile : tile + 1]
            copy = pltpu.make_async_copy(mean_ref.at[where], out_ref.at[where], sems.at[pair, k])
            copy.start()
            copies.append(copy)
    for copy in copies:
        copy.wait()


def finish_tiles(same_parts, other_parts, begun, number, middle):
    pairs, rows, lanes = other_parts[0].shape[1:]
    entries = len(other_parts) * pairs * (rows - META)
    return pl.pallas_call(
        functools.partial(finish_tiles_kernel, len(other_parts)),
        out_shape=jax.ShapeDtypeStruct((BUCKET, lanes), jnp.float32),
        in_specs=[vmem_spec()] * (2 * len(other_parts) + 5),
        out_specs=hbm_spec(),
        scratch_shapes=[
            pltpu.VMEM((BUCKET, lanes), jnp.float32),
            pltpu.VMEM((TILE, lanes), jnp.float32),
            pltpu.VMEM((TILE, entries), jnp.bfloat16),
            pltpu.VMEM((entries, lanes), jnp.bfloat16),
            pltpu.VMEM((TILE, lanes), jnp.float32),
            pltpu.SemaphoreType.DMA((BUCKET // (2 * TILE), 2)),
        ],
        cost_estimate=dense_cost(entries, lanes, 2.0),
        compiler_params=grant(16 * MIB),
        name="finish_tiles",
    )(*same_parts, *other_parts, begun, number, *middle)


def by_pairs(values, slots, counts, groups):
    members = values.shape[0]
    pairs = members // 2

    def swap(array, axis, size, by):
        return lax.ppermute(array, axis, [(i, i ^ by) for i in range(size)])

    sent = pack(values, slots, counts, groups, True)
    mine = [sent[0]] + [swap(sent[k], "mem", members, 2 * k) for k in range(1, pairs)]
    mine = jnp.stack(mine, axis=1)
    same = [mine] + [swap(mine, "grp", groups, k) for k in range(1, groups)]
    other = [swap(part, "mem", members, 1) for part in same]
    first = [same[0], other[0]]
    begun = begin_answer(first)
    early = dense_prepare(first)
    sums = begin_tiles(first, early)
    begun = more_answer(same[1:], begun)
    prepared = dense_prepare(same[1:])
    answers = finish_answer(other[1:], begun)
    averaged = finish_tiles(same[1:], other[1:], sums, early[2], prepared)
    back = [answers[0]] + [swap(answers[k], "mem", members, 2 * k) for k in range(1, pairs)]
    return averaged, place(back)


def by_all(values, slots, counts, groups):
    members = values.shape[0]
    (lists,) = pack(values, slots, counts, groups, False)
    got = lax.all_to_all(lists, ("grp", "mem"), split_axis=0, concat_axis=0, tiled=True)
    back = answer(got, members)
    returned = lax.all_to_all(back, "mem", split_axis=0, concat_axis=0, tiled=True)
    return dense(got), returned


def per_device(groups, values, slots, counts):
    members, capacity, lanes = values.shape[1:]
    entries = groups * members * capacity
    few = members == 8 and groups in (2, 4, 8) and entries <= 2048 and 4 * capacity == lanes
    tiles = BUCKET % (2 * TILE) == 0 and BUCKET // TILE <= lanes
    move = by_pairs if few and tiles else by_all
    averaged, returned = move(values[0], slots[0], counts, groups)
    return (averaged, returned[None])


def one_step(groups, values, slots, counts):
    return per_device(groups, values, slots, counts)


def solution(mesh):
    return jax.shard_map(
        functools.partial(one_step, mesh.shape["grp"]),
        mesh=mesh,
        in_specs=(
            P(("grp", "mem"), None, None, None),
            P(("grp", "mem"), None, None),
            P(("grp", "mem"), None),
        ),
        out_specs=(P("mem", None), P(("grp", "mem"), None, None, None)),
        check_vma=False,
    )
```

```python
import functools
import math

import jax
import jax.numpy as jnp
from jax import lax
from jax.experimental import pallas as pl
from jax.experimental.pallas import tpu as pltpu
from jax.sharding import PartitionSpec as P


BUCKET = 7168
DIGIT = 256
TILE = 512
META = 8
MIB = 2**20


def vmem_spec():
    return pl.BlockSpec(memory_space=pltpu.VMEM)


def hbm_spec():
    return pl.BlockSpec(memory_space=pltpu.HBM)


def grant(size):
    return pltpu.CompilerParams(vmem_limit_bytes=size)


def place_in_list_kernel(out_ref):
    out_ref[...] = lax.broadcasted_iota(jnp.int32, out_ref.shape, 1).astype(jnp.float32)


def meta_rows(slots_ref, counts_ref, place_ref, lanes, buckets):
    members, capacity = slots_ref.shape
    shape = (members, members)
    diagonal = lax.broadcasted_iota(jnp.int32, shape, 0) == lax.broadcasted_iota(jnp.int32, shape, 1)
    count = jnp.sum(jnp.where(diagonal, counts_ref[...].astype(jnp.float32), 0.0), axis=1, keepdims=True)
    slot = slots_ref[...]
    live = place_ref[...] < count
    high = jnp.where(live, (slot // DIGIT).astype(jnp.float32), -1.0)
    low = jnp.where(live, (slot % DIGIT).astype(jnp.float32), 0.0)
    repeats = lanes // capacity
    high = jnp.concatenate([high] * repeats, axis=1)
    low = jnp.concatenate([low] * repeats, axis=1)
    row = lax.broadcasted_iota(jnp.int32, (members, META, lanes), 1)
    row = row - 2 * lax.rem(lax.broadcasted_iota(jnp.int32, row.shape, 0), buckets)
    meta = jnp.where(row == 0, high[:, None, :], jnp.where(row == 1, low[:, None, :], 0.0))
    return meta.astype(jnp.bfloat16)


def pack_groups_kernel(values_ref, slots_ref, counts_ref, place_ref, out_ref):
    members, capacity, lanes = values_ref.shape
    meta = meta_rows(slots_ref, counts_ref, place_ref, lanes, 1)
    for group in range(out_ref.shape[0] // members):
        rows = pl.ds(group * members, members)
        out_ref[rows, pl.ds(0, capacity), :] = values_ref[...]
        out_ref[rows, pl.ds(capacity, META), :] = meta


def pack_pairs_kernel(values_ref, slots_ref, counts_ref, place_ref, *out_and_scratch):
    *out_refs, meta_ref = out_and_scratch
    capacity, lanes = values_ref.shape[1:]
    meta_ref[...] = meta_rows(slots_ref, counts_ref, place_ref, lanes, 2)
    pair = lax.div(lax.axis_index("mem"), 2)
    for k, out_ref in enumerate(out_refs):
        first = 2 * lax.bitwise_xor(pair, jnp.int32(k))
        for bucket in range(2):
            out_ref[pl.ds(bucket * capacity, capacity), :] = values_ref[first + bucket]
        out_ref[pl.ds(2 * capacity, META), :] = meta_ref[first] + meta_ref[first + 1]


def pack(values, slots, counts, groups, paired):
    members, capacity, lanes = values.shape
    place_in_list = pl.pallas_call(
        place_in_list_kernel,
        out_shape=jax.ShapeDtypeStruct(slots.shape, jnp.float32),
        out_specs=vmem_spec(),
        cost_estimate=pl.CostEstimate(flops=2 * 10**9, bytes_accessed=16 * 10**6, transcendentals=0),
        compiler_params=grant(MIB),
        name="place_in_list",
    )()
    if paired:
        shape = jax.ShapeDtypeStruct((2 * capacity + META, lanes), jnp.bfloat16)
        kernel, out_shape = pack_pairs_kernel, [shape] * (members // 2)
        scratch = [pltpu.VMEM((members, META, lanes), jnp.bfloat16)]
    else:
        shape = jax.ShapeDtypeStruct((groups * members, capacity + META, lanes), jnp.bfloat16)
        kernel, out_shape = pack_groups_kernel, [shape]
        scratch = []
    return pl.pallas_call(
        kernel,
        out_shape=out_shape,
        in_specs=[vmem_spec()] * 4,
        out_specs=[vmem_spec()] * len(out_shape),
        scratch_shapes=scratch,
        compiler_params=grant(8 * MIB),
        name="pack",
    )(values, slots, counts, place_in_list)


def capacity_of(view):
    ref, bucket = view
    rows = ref.shape[1] - META
    return rows if bucket is None else rows // 2


def digits_of(views):
    high, low = [], []
    for ref, bucket in views:
        meta = ref[:, pl.ds(ref.shape[1] - META, META), :].astype(jnp.float32)
        if bucket is None or isinstance(bucket, int):
            at = 2 * (bucket or 0)
            high.append(meta[:, at, :])
            low.append(meta[:, at + 1, :])
        else:
            high.append(jnp.where(bucket == 0, meta[:, 0, :], meta[:, 2, :]))
            low.append(jnp.where(bucket == 0, meta[:, 1, :], meta[:, 3, :]))
    return jnp.concatenate(high, axis=0), jnp.concatenate(low, axis=0)


def entries_of(views):
    capacity, lanes = capacity_of(views[0]), views[0][0].shape[2]

    def rows(bucket):
        if bucket is None or isinstance(bucket, int):
            return pl.ds((bucket or 0) * capacity, capacity)
        return pl.ds(pl.multiple_of(bucket * capacity, capacity), capacity)

    return jnp.concatenate([ref[:, rows(bucket), :].reshape(-1, lanes) for ref, bucket in views], axis=0)


def as_row(digit, capacity):
    lists, lanes = digit.shape
    per_block = lanes // capacity
    part = lax.broadcasted_iota(jnp.int32, (1, lanes), 1) // capacity
    blocks = []
    for block in range(lists // per_block):
        row = digit[block * per_block : block * per_block + 1]
        for k in range(1, per_block):
            at = block * per_block + k
            row = jnp.where(part == k, digit[at : at + 1], row)
        blocks.append(row)
    return jnp.concatenate(blocks, axis=1)


def as_column(digit, capacity):
    lists, lanes = digit.shape
    shape = (lists, capacity, lanes)
    here = lax.broadcasted_iota(jnp.int32, shape, 2) == lax.broadcasted_iota(jnp.int32, shape, 1)
    picked = jnp.where(here, digit[:, None, :], 0.0).astype(jnp.bfloat16).reshape(lists * capacity, lanes)
    return jnp.dot(picked, jnp.ones((lanes, lanes), jnp.bfloat16), preferred_element_type=jnp.float32)


def keys_of(views):
    high, low = digits_of(views)
    return as_row(high * DIGIT + low, capacity_of(views[0]))


def asked_column(asking):
    capacity = capacity_of(asking[0])
    high, low = digits_of(asking)
    column = as_column(high, capacity) * DIGIT + as_column(low, capacity)
    return jnp.where(column < 0.0, -1.0, column)


def matching_sums(column, key, entries):
    lanes = entries.shape[1]
    onehot = jnp.concatenate(
        [
            (column == key[:, at : at + lanes]).astype(jnp.float32).astype(jnp.bfloat16)
            for at in range(0, entries.shape[0], lanes)
        ],
        axis=1,
    )
    sums = jnp.dot(onehot, entries, preferred_element_type=jnp.float32)
    return sums, jnp.dot(onehot, jnp.ones_like(entries), preferred_element_type=jnp.float32)


def answer_kernel(lists_ref, out_ref, key_ref):
    members = out_ref.shape[0]
    step = math.gcd(members, 8)
    key_ref[...] = keys_of([(lists_ref, None)])
    first = lax.axis_index("grp") * members

    @pl.loop(0, members, step=step)
    def _(at):
        asking = (lists_ref.at[pl.ds(first + at, step)], None)
        sums, count = matching_sums(asked_column([asking]), key_ref[...], entries_of([(lists_ref, None)]))
        mean = sums / jnp.maximum(count, 1.0)
        out_ref[pl.ds(at, step)] = mean.astype(jnp.bfloat16).reshape(step, *out_ref.shape[1:])


def answer(lists, members):
    senders, rows, lanes = lists.shape
    capacity = rows - META
    entries = senders * capacity
    return pl.pallas_call(
        answer_kernel,
        out_shape=jax.ShapeDtypeStruct((members, capacity, lanes), jnp.bfloat16),
        in_specs=[vmem_spec()],
        out_specs=vmem_spec(),
        scratch_shapes=[pltpu.VMEM((1, entries), jnp.float32)],
        compiler_params=grant(48 * entries * lanes),
        name="answer",
    )(lists)


def partial_answer(refs, bucket, column_ref):
    views = [(ref, bucket) for ref in refs]
    return matching_sums(column_ref[bucket], keys_of(views), entries_of(views))


def begin_answer_kernel(*refs):
    *in_refs, column_ref, sums_ref, count_ref = refs
    for bucket in range(2):
        column_ref[bucket] = asked_column([(in_refs[0], bucket)])
        sums_ref[bucket], count_ref[bucket] = partial_answer(in_refs, bucket, column_ref)


def more_answer_kernel(*refs):
    *in_refs, column_ref, sums_ref, count_ref, new_sums_ref, new_count_ref = refs
    for bucket in range(2):
        sums, number = partial_answer(in_refs, bucket, column_ref)
        new_sums_ref[bucket] = sums_ref[bucket] + sums
        new_count_ref[bucket] = count_ref[bucket] + number


def finish_answer_kernel(count, *refs):
    in_refs, (column_ref, sums_ref, count_ref), out_refs = refs[:count], refs[count : count + 3], refs[count + 3 :]
    for bucket in range(2):
        sums, number = partial_answer(in_refs, bucket, column_ref)
        mean = (sums_ref[bucket] + sums) / jnp.maximum(count_ref[bucket] + number, 1.0)
        mean = mean.astype(jnp.bfloat16).reshape(len(out_refs), *out_refs[0].shape[1:])
        for k, out_ref in enumerate(out_refs):
            out_ref[bucket] = mean[k]


def run_answer(kernel, out_shape, operands):
    return pl.pallas_call(
        kernel,
        out_shape=out_shape,
        in_specs=[vmem_spec()] * len(operands),
        out_specs=[vmem_spec()] * len(out_shape),
        compiler_params=grant(8 * MIB),
    )(*operands)


def begin_answer(parts):
    pairs, rows, lanes = parts[0].shape
    partial = jax.ShapeDtypeStruct((2, pairs * (rows - META) // 2, lanes), jnp.float32)
    return run_answer(begin_answer_kernel, [partial] * 3, parts)


def more_answer(parts, begun):
    partial = jax.ShapeDtypeStruct(begun[0].shape, jnp.float32)
    return [begun[0], *run_answer(more_answer_kernel, [partial] * 2, [*parts, *begun])]


def finish_answer(parts, begun):
    pairs, rows, lanes = parts[0].shape
    shape = jax.ShapeDtypeStruct((2, (rows - META) // 2, lanes), jnp.bfloat16)
    kernel = functools.partial(finish_answer_kernel, len(parts))
    return run_answer(kernel, [shape] * pairs, [*parts, *begun])


def place_kernel(*refs):
    *parts, out_ref, sems = refs
    pair = lax.div(lax.axis_index("mem"), 2)
    copies = []
    for k, part in enumerate(parts):
        rows = pl.ds(2 * lax.bitwise_xor(pair, jnp.int32(k)), 2)
        copies.append(pltpu.make_async_copy(part, out_ref.at[rows], sems.at[k]))
    for copy in copies:
        copy.start()
    for copy in copies:
        copy.wait()


def place(parts):
    two, capacity, lanes = parts[0].shape
    return pl.pallas_call(
        place_kernel,
        out_shape=jax.ShapeDtypeStruct((two * len(parts), capacity, lanes), jnp.bfloat16),
        in_specs=[vmem_spec()] * len(parts),
        out_specs=hbm_spec(),
        scratch_shapes=[pltpu.SemaphoreType.DMA((len(parts),))],
        compiler_params=grant(2 * MIB),
        name="place",
    )(*parts)


def dense_cost(entries, lanes, share=1.0):
    flops = int(2 * BUCKET * entries * lanes * share)
    return pl.CostEstimate(flops=flops, bytes_accessed=int(4 * BUCKET * lanes * share), transcendentals=0)


def dense_kernel(lists_ref, out_ref, key_ref):
    @pl.when(pl.program_id(0) == 0)
    def _():
        key_ref[...] = keys_of([(lists_ref, None)])

    tile = out_ref.shape[0]
    wanted = (lax.broadcasted_iota(jnp.int32, (tile, 1), 0) + pl.program_id(0) * tile).astype(jnp.float32)
    onehot = (wanted == key_ref[...]).astype(jnp.float32).astype(jnp.bfloat16)
    entries = entries_of([(lists_ref, None)])
    sums = jnp.dot(onehot, entries, preferred_element_type=jnp.float32)
    count = jnp.dot(onehot, jnp.ones_like(entries), preferred_element_type=jnp.float32)
    out_ref[...] = sums / jnp.maximum(count, 1.0)


def dense(lists):
    senders, rows, lanes = lists.shape
    entries = senders * (rows - META)
    tile = math.gcd(BUCKET, 512)
    return pl.pallas_call(
        dense_kernel,
        grid=(BUCKET // tile,),
        out_shape=jax.ShapeDtypeStruct((BUCKET, lanes), jnp.float32),
        in_specs=[vmem_spec()],
        out_specs=pl.BlockSpec((tile, lanes), lambda i: (i, 0)),
        scratch_shapes=[pltpu.VMEM((1, entries), jnp.float32)],
        cost_estimate=dense_cost(entries, lanes),
        name="dense",
    )(lists)


def own_bucket(refs):
    bucket = lax.rem(lax.axis_index("mem"), 2)
    return [(ref, bucket) for ref in refs]


def prepare_tiles(views, same_ref, tile_ref, number_ref):
    capacity, lanes = capacity_of(views[0]), tile_ref.shape[1]
    entries = same_ref.shape[1]
    ratio = TILE // DIGIT
    high, low = digits_of(views)
    tile = jnp.floor(high * (1.0 / ratio))
    low_row = as_row(low + DIGIT * (high - ratio * tile), capacity)
    wanted = lax.broadcasted_iota(jnp.int32, (TILE, lanes), 0).astype(jnp.float32)
    for at in range(0, entries, lanes):
        same = (wanted == low_row[:, at : at + lanes]).astype(jnp.float32)
        same_ref[:, at : at + lanes] = same.astype(jnp.bfloat16)
    tile_column = as_column(tile, capacity)
    tile_ref[...] = tile_column.astype(jnp.bfloat16)
    lane = lax.broadcasted_iota(jnp.int32, (entries, lanes), 1).astype(jnp.float32)
    in_tile = (tile_column == lane).astype(jnp.float32).astype(jnp.bfloat16)
    number_ref[...] = jnp.dot(same_ref[...], in_tile, preferred_element_type=jnp.float32)


def dense_prepare_kernel(*refs):
    *in_refs, same_ref, tile_ref, number_ref = refs
    prepare_tiles(own_bucket(in_refs), same_ref, tile_ref, number_ref)


def dense_prepare(parts):
    pairs, rows, lanes = parts[0].shape
    entries = len(parts) * pairs * (rows - META) // 2
    return pl.pallas_call(
        dense_prepare_kernel,
        out_shape=[
            jax.ShapeDtypeStruct((TILE, entries), jnp.bfloat16),
            jax.ShapeDtypeStruct((entries, lanes), jnp.bfloat16),
            jax.ShapeDtypeStruct((TILE, lanes), jnp.float32),
        ],
        in_specs=[vmem_spec()] * len(parts),
        out_specs=[vmem_spec()] * 3,
        compiler_params=grant(8 * MIB),
        name="dense_prepare",
    )(*parts)


def pair_sums(pair, views, same_refs, tile_refs):
    values = entries_of(views)
    tile_of = jnp.concatenate([ref[...] for ref in tile_refs], axis=0)
    same = jnp.concatenate([ref[...] for ref in same_refs], axis=1)
    zero = jnp.zeros_like(values)
    picked = jnp.concatenate([jnp.where(tile_of == 2 * pair + k, values, zero) for k in range(2)], axis=1)
    return jnp.dot(same, picked, preferred_element_type=jnp.float32)


def begin_tiles_kernel(*refs):
    *in_refs, same_ref, tile_ref, out_ref = refs
    views = own_bucket(in_refs)
    lanes = out_ref.shape[1]
    for pair in range(BUCKET // (2 * TILE)):
        sums = pair_sums(pair, views, [same_ref], [tile_ref])
        for k in range(2):
            out_ref[pl.ds((2 * pair + k) * TILE, TILE), :] = sums[:, k * lanes : (k + 1) * lanes]


def begin_tiles(parts, prepared):
    lanes = parts[0].shape[2]
    return pl.pallas_call(
        begin_tiles_kernel,
        out_shape=jax.ShapeDtypeStruct((BUCKET, lanes), jnp.float32),
        in_specs=[vmem_spec()] * (len(parts) + 2),
        out_specs=vmem_spec(),
        compiler_params=grant(8 * MIB),
        name="begin_tiles",
    )(*parts, *prepared[:2])


def finish_tiles_kernel(count, *refs):
    same_parts, other_parts = refs[:count], refs[count : 2 * count]
    begun_ref, number_ref, *middle = refs[2 * count : 2 * count + 5]
    out_ref, mean_ref, inverse_ref, same_ref, tile_ref, last_ref, sems = refs[2 * count + 5 :]
    prepare_tiles(own_bucket(other_parts), same_ref, tile_ref, last_ref)
    views = own_bucket(same_parts + other_parts)
    lanes = mean_ref.shape[1]
    inverse_ref[...] = 1.0 / jnp.maximum(number_ref[...] + middle[2][...] + last_ref[...], 1.0)
    copies = []
    for pair in range(sems.shape[0]):
        sums = pair_sums(pair, views, [middle[0], same_ref], [middle[1], tile_ref])
        for k in range(2):
            tile = 2 * pair + k
            where = pl.ds(tile * TILE, TILE)
            total = begun_ref[where, :] + sums[:, k * lanes : (k + 1) * lanes]
            mean_ref[where, :] = total * inverse_ref[:, tile : tile + 1]
            copy = pltpu.make_async_copy(mean_ref.at[where], out_ref.at[where], sems.at[pair, k])
            copy.start()
            copies.append(copy)
    for copy in copies:
        copy.wait()


def finish_tiles(same_parts, other_parts, begun, number, middle):
    pairs, rows, lanes = other_parts[0].shape
    entries = len(other_parts) * pairs * (rows - META) // 2
    return pl.pallas_call(
        functools.partial(finish_tiles_kernel, len(other_parts)),
        out_shape=jax.ShapeDtypeStruct((BUCKET, lanes), jnp.float32),
        in_specs=[vmem_spec()] * (2 * len(other_parts) + 5),
        out_specs=hbm_spec(),
        scratch_shapes=[
            pltpu.VMEM((BUCKET, lanes), jnp.float32),
            pltpu.VMEM((TILE, lanes), jnp.float32),
            pltpu.VMEM((TILE, entries), jnp.bfloat16),
            pltpu.VMEM((entries, lanes), jnp.bfloat16),
            pltpu.VMEM((TILE, lanes), jnp.float32),
            pltpu.SemaphoreType.DMA((BUCKET // (2 * TILE), 2)),
        ],
        cost_estimate=dense_cost(entries, lanes, 2.0),
        compiler_params=grant(16 * MIB),
        name="finish_tiles",
    )(*same_parts, *other_parts, begun, number, *middle)


def by_pairs(values, slots, counts, groups):
    members = values.shape[0]
    pairs = members // 2

    def swap(array, axis, size, by):
        return lax.ppermute(array, axis, [(i, i ^ by) for i in range(size)])

    sent = pack(values, slots, counts, groups, True)
    mine = [sent[0]] + [swap(sent[k], "mem", members, 2 * k) for k in range(1, pairs)]
    mine = jnp.stack(mine, axis=0)
    same = [mine] + [swap(mine, "grp", groups, k) for k in range(1, groups)]
    other = [swap(part, "mem", members, 1) for part in same]
    first = [same[0], other[0]]
    begun = begin_answer(first)
    early = dense_prepare(first)
    sums = begin_tiles(first, early)
    begun = more_answer(same[1:], begun)
    prepared = dense_prepare(same[1:])
    answers = finish_answer(other[1:], begun)
    averaged = finish_tiles(same[1:], other[1:], sums, early[2], prepared)
    back = [answers[0]] + [swap(answers[k], "mem", members, 2 * k) for k in range(1, pairs)]
    return averaged, place(back)


def by_all(values, slots, counts, groups):
    members = values.shape[0]
    (lists,) = pack(values, slots, counts, groups, False)
    got = lax.all_to_all(lists, ("grp", "mem"), split_axis=0, concat_axis=0, tiled=True)
    back = answer(got, members)
    returned = lax.all_to_all(back, "mem", split_axis=0, concat_axis=0, tiled=True)
    return dense(got), returned


def per_device(groups, values, slots, counts):
    members, capacity, lanes = values.shape[1:]
    entries = groups * members * capacity
    few = members == 8 and groups in (2, 4, 8) and entries <= 2048 and 4 * capacity == lanes
    tiles = BUCKET % (2 * TILE) == 0 and BUCKET // TILE <= lanes
    move = by_pairs if few and tiles else by_all
    averaged, returned = move(values[0], slots[0], counts, groups)
    return (averaged, returned[None])


def one_step(groups, values, slots, counts):
    return per_device(groups, values, slots, counts)


def solution(mesh):
    return jax.shard_map(
        functools.partial(one_step, mesh.shape["grp"]),
        mesh=mesh,
        in_specs=(
            P(("grp", "mem"), None, None, None),
            P(("grp", "mem"), None, None),
            P(("grp", "mem"), None),
        ),
        out_specs=(P("mem", None), P(("grp", "mem"), None, None, None)),
        check_vma=False,
    )
```

```python
import functools
import math

import jax
import jax.numpy as jnp
from jax import lax
from jax.experimental import pallas as pl
from jax.experimental.pallas import tpu as pltpu
from jax.sharding import PartitionSpec as P


BUCKET = 7168
DIGIT = 256
TILE = 512
META = 8
MIB = 2**20


def vmem_spec():
    return pl.BlockSpec(memory_space=pltpu.VMEM)


def hbm_spec():
    return pl.BlockSpec(memory_space=pltpu.HBM)


def grant(size):
    return pltpu.CompilerParams(vmem_limit_bytes=size)


def place_in_list_kernel(out_ref):
    out_ref[...] = lax.broadcasted_iota(jnp.int32, out_ref.shape, 1).astype(jnp.float32)


def meta_rows(slots_ref, counts_ref, place_ref, lanes, buckets):
    members, capacity = slots_ref.shape
    shape = (members, members)
    diagonal = lax.broadcasted_iota(jnp.int32, shape, 0) == lax.broadcasted_iota(jnp.int32, shape, 1)
    count = jnp.sum(jnp.where(diagonal, counts_ref[...].astype(jnp.float32), 0.0), axis=1, keepdims=True)
    slot = slots_ref[...]
    live = place_ref[...] < count
    high = jnp.where(live, (slot // DIGIT).astype(jnp.float32), -1.0)
    low = jnp.where(live, (slot % DIGIT).astype(jnp.float32), 0.0)
    repeats = lanes // capacity
    high = jnp.concatenate([high] * repeats, axis=1)
    low = jnp.concatenate([low] * repeats, axis=1)
    row = lax.broadcasted_iota(jnp.int32, (members, META, lanes), 1)
    row = row - 2 * lax.rem(lax.broadcasted_iota(jnp.int32, row.shape, 0), buckets)
    meta = jnp.where(row == 0, high[:, None, :], jnp.where(row == 1, low[:, None, :], 0.0))
    return meta.astype(jnp.bfloat16)


def pack_groups_kernel(values_ref, slots_ref, counts_ref, place_ref, out_ref):
    members, capacity, lanes = values_ref.shape
    meta = meta_rows(slots_ref, counts_ref, place_ref, lanes, 1)
    for group in range(out_ref.shape[0] // members):
        rows = pl.ds(group * members, members)
        out_ref[rows, pl.ds(0, capacity), :] = values_ref[...]
        out_ref[rows, pl.ds(capacity, META), :] = meta


def pack_pairs_kernel(values_ref, slots_ref, counts_ref, place_ref, *out_and_scratch):
    *out_refs, meta_ref = out_and_scratch
    capacity, lanes = values_ref.shape[1:]
    meta_ref[...] = meta_rows(slots_ref, counts_ref, place_ref, lanes, 2)
    pair = lax.div(lax.axis_index("mem"), 2)
    for k, out_ref in enumerate(out_refs):
        first = 2 * lax.bitwise_xor(pair, jnp.int32(k))
        for bucket in range(2):
            out_ref[pl.ds(bucket * capacity, capacity), :] = values_ref[first + bucket]
        out_ref[pl.ds(2 * capacity, META), :] = meta_ref[first] + meta_ref[first + 1]


def pack(values, slots, counts, groups, paired):
    members, capacity, lanes = values.shape
    place_in_list = pl.pallas_call(
        place_in_list_kernel,
        out_shape=jax.ShapeDtypeStruct(slots.shape, jnp.float32),
        out_specs=vmem_spec(),
        cost_estimate=pl.CostEstimate(flops=2 * 10**9, bytes_accessed=16 * 10**6, transcendentals=0),
        compiler_params=grant(MIB),
        name="place_in_list",
    )()
    if paired:
        shape = jax.ShapeDtypeStruct((2 * capacity + META, lanes), jnp.bfloat16)
        kernel, out_shape = pack_pairs_kernel, [shape] * (members // 2)
        scratch = [pltpu.VMEM((members, META, lanes), jnp.bfloat16)]
    else:
        shape = jax.ShapeDtypeStruct((groups * members, capacity + META, lanes), jnp.bfloat16)
        kernel, out_shape = pack_groups_kernel, [shape]
        scratch = []
    return pl.pallas_call(
        kernel,
        out_shape=out_shape,
        in_specs=[vmem_spec()] * 4,
        out_specs=[vmem_spec()] * len(out_shape),
        scratch_shapes=scratch,
        compiler_params=grant(8 * MIB),
        name="pack",
    )(values, slots, counts, place_in_list)


def capacity_of(view):
    ref, bucket = view
    rows = ref.shape[1] - META
    return rows if bucket is None else rows // 2


def digits_of(views):
    high, low = [], []
    for ref, bucket in views:
        meta = ref[:, pl.ds(ref.shape[1] - META, META), :].astype(jnp.float32)
        if bucket is None or isinstance(bucket, int):
            at = 2 * (bucket or 0)
            high.append(meta[:, at, :])
            low.append(meta[:, at + 1, :])
        else:
            high.append(jnp.where(bucket == 0, meta[:, 0, :], meta[:, 2, :]))
            low.append(jnp.where(bucket == 0, meta[:, 1, :], meta[:, 3, :]))
    return jnp.concatenate(high, axis=0), jnp.concatenate(low, axis=0)


def entries_of(views):
    capacity, lanes = capacity_of(views[0]), views[0][0].shape[2]

    def rows(bucket):
        if bucket is None or isinstance(bucket, int):
            return pl.ds((bucket or 0) * capacity, capacity)
        return pl.ds(pl.multiple_of(bucket * capacity, capacity), capacity)

    return jnp.concatenate([ref[:, rows(bucket), :].reshape(-1, lanes) for ref, bucket in views], axis=0)


def as_row(digit, capacity):
    lists, lanes = digit.shape
    per_block = lanes // capacity
    part = lax.broadcasted_iota(jnp.int32, (1, lanes), 1) // capacity
    blocks = []
    for block in range(lists // per_block):
        row = digit[block * per_block : block * per_block + 1]
        for k in range(1, per_block):
            at = block * per_block + k
            row = jnp.where(part == k, digit[at : at + 1], row)
        blocks.append(row)
    return jnp.concatenate(blocks, axis=1)


def as_column(digit, capacity):
    lists, lanes = digit.shape
    shape = (lists, capacity, lanes)
    here = lax.broadcasted_iota(jnp.int32, shape, 2) == lax.broadcasted_iota(jnp.int32, shape, 1)
    picked = jnp.where(here, digit[:, None, :], 0.0).astype(jnp.bfloat16).reshape(lists * capacity, lanes)
    return jnp.dot(picked, jnp.ones((lanes, lanes), jnp.bfloat16), preferred_element_type=jnp.float32)


def keys_of(views):
    high, low = digits_of(views)
    return as_row(high * DIGIT + low, capacity_of(views[0]))


def asked_column(asking):
    capacity = capacity_of(asking[0])
    high, low = digits_of(asking)
    column = as_column(high, capacity) * DIGIT + as_column(low, capacity)
    return jnp.where(column < 0.0, -1.0, column)


def matching_sums(column, key, entries):
    lanes = entries.shape[1]
    onehot = jnp.concatenate(
        [
            (column == key[:, at : at + lanes]).astype(jnp.float32).astype(jnp.bfloat16)
            for at in range(0, entries.shape[0], lanes)
        ],
        axis=1,
    )
    sums = jnp.dot(onehot, entries, preferred_element_type=jnp.float32)
    return sums, jnp.dot(onehot, jnp.ones_like(entries), preferred_element_type=jnp.float32)


def answer_kernel(lists_ref, out_ref, key_ref):
    members = out_ref.shape[0]
    step = math.gcd(members, 8)
    key_ref[...] = keys_of([(lists_ref, None)])
    first = lax.axis_index("grp") * members

    @pl.loop(0, members, step=step)
    def _(at):
        asking = (lists_ref.at[pl.ds(first + at, step)], None)
        sums, count = matching_sums(asked_column([asking]), key_ref[...], entries_of([(lists_ref, None)]))
        mean = sums / jnp.maximum(count, 1.0)
        out_ref[pl.ds(at, step)] = mean.astype(jnp.bfloat16).reshape(step, *out_ref.shape[1:])


def answer(lists, members):
    senders, rows, lanes = lists.shape
    capacity = rows - META
    entries = senders * capacity
    return pl.pallas_call(
        answer_kernel,
        out_shape=jax.ShapeDtypeStruct((members, capacity, lanes), jnp.bfloat16),
        in_specs=[vmem_spec()],
        out_specs=vmem_spec(),
        scratch_shapes=[pltpu.VMEM((1, entries), jnp.float32)],
        compiler_params=grant(48 * entries * lanes),
        name="answer",
    )(lists)


def partial_answer(refs, bucket, column_ref):
    views = [(ref, bucket) for ref in refs]
    return matching_sums(column_ref[bucket], keys_of(views), entries_of(views))


def begin_answer_kernel(*refs):
    *in_refs, column_ref, sums_ref, count_ref = refs
    for bucket in range(2):
        column_ref[bucket] = asked_column([(in_refs[0], bucket)])
        sums_ref[bucket], count_ref[bucket] = partial_answer(in_refs, bucket, column_ref)


def more_answer_kernel(*refs):
    *in_refs, column_ref, sums_ref, count_ref, new_sums_ref, new_count_ref = refs
    for bucket in range(2):
        sums, number = partial_answer(in_refs, bucket, column_ref)
        new_sums_ref[bucket] = sums_ref[bucket] + sums
        new_count_ref[bucket] = count_ref[bucket] + number


def finish_answer_kernel(count, *refs):
    in_refs, (column_ref, sums_ref, count_ref), out_refs = refs[:count], refs[count : count + 3], refs[count + 3 :]
    for bucket in range(2):
        sums, number = partial_answer(in_refs, bucket, column_ref)
        mean = (sums_ref[bucket] + sums) / jnp.maximum(count_ref[bucket] + number, 1.0)
        mean = mean.astype(jnp.bfloat16).reshape(len(out_refs), *out_refs[0].shape[1:])
        for k, out_ref in enumerate(out_refs):
            out_ref[bucket] = mean[k]


def run_answer(kernel, out_shape, operands):
    return pl.pallas_call(
        kernel,
        out_shape=out_shape,
        in_specs=[vmem_spec()] * len(operands),
        out_specs=[vmem_spec()] * len(out_shape),
        compiler_params=grant(8 * MIB),
    )(*operands)


def begin_answer(parts):
    pairs, rows, lanes = parts[0].shape
    partial = jax.ShapeDtypeStruct((2, pairs * (rows - META) // 2, lanes), jnp.float32)
    return run_answer(begin_answer_kernel, [partial] * 3, parts)


def more_answer(parts, begun):
    partial = jax.ShapeDtypeStruct(begun[0].shape, jnp.float32)
    return [begun[0], *run_answer(more_answer_kernel, [partial] * 2, [*parts, *begun])]


def finish_answer(parts, begun):
    pairs, rows, lanes = parts[0].shape
    shape = jax.ShapeDtypeStruct((2, (rows - META) // 2, lanes), jnp.bfloat16)
    kernel = functools.partial(finish_answer_kernel, len(parts))
    return run_answer(kernel, [shape] * pairs, [*parts, *begun])


def place_kernel(*refs):
    *parts, out_ref, sems = refs
    pair = lax.div(lax.axis_index("mem"), 2)
    copies = []
    for k, part in enumerate(parts):
        rows = pl.ds(2 * lax.bitwise_xor(pair, jnp.int32(k)), 2)
        copies.append(pltpu.make_async_copy(part, out_ref.at[rows], sems.at[k]))
    for copy in copies:
        copy.start()
    for copy in copies:
        copy.wait()


def place(parts):
    two, capacity, lanes = parts[0].shape
    return pl.pallas_call(
        place_kernel,
        out_shape=jax.ShapeDtypeStruct((two * len(parts), capacity, lanes), jnp.bfloat16),
        in_specs=[vmem_spec()] * len(parts),
        out_specs=hbm_spec(),
        scratch_shapes=[pltpu.SemaphoreType.DMA((len(parts),))],
        compiler_params=grant(2 * MIB),
        name="place",
    )(*parts)


def dense_cost(entries, lanes, share=1.0):
    flops = int(2 * BUCKET * entries * lanes * share)
    return pl.CostEstimate(flops=flops, bytes_accessed=int(4 * BUCKET * lanes * share), transcendentals=0)


def dense_kernel(lists_ref, out_ref, key_ref):
    @pl.when(pl.program_id(0) == 0)
    def _():
        key_ref[...] = keys_of([(lists_ref, None)])

    tile = out_ref.shape[0]
    wanted = (lax.broadcasted_iota(jnp.int32, (tile, 1), 0) + pl.program_id(0) * tile).astype(jnp.float32)
    onehot = (wanted == key_ref[...]).astype(jnp.float32).astype(jnp.bfloat16)
    entries = entries_of([(lists_ref, None)])
    sums = jnp.dot(onehot, entries, preferred_element_type=jnp.float32)
    count = jnp.dot(onehot, jnp.ones_like(entries), preferred_element_type=jnp.float32)
    out_ref[...] = sums / jnp.maximum(count, 1.0)


def dense(lists):
    senders, rows, lanes = lists.shape
    entries = senders * (rows - META)
    tile = math.gcd(BUCKET, 512)
    return pl.pallas_call(
        dense_kernel,
        grid=(BUCKET // tile,),
        out_shape=jax.ShapeDtypeStruct((BUCKET, lanes), jnp.float32),
        in_specs=[vmem_spec()],
        out_specs=pl.BlockSpec((tile, lanes), lambda i: (i, 0)),
        scratch_shapes=[pltpu.VMEM((1, entries), jnp.float32)],
        cost_estimate=dense_cost(entries, lanes),
        name="dense",
    )(lists)


def own_bucket(refs):
    bucket = lax.rem(lax.axis_index("mem"), 2)
    return [(ref, bucket) for ref in refs]


def prepare_tiles(views, same_ref, tile_ref, number_ref):
    capacity, lanes = capacity_of(views[0]), tile_ref.shape[1]
    entries = same_ref.shape[1]
    ratio = TILE // DIGIT
    high, low = digits_of(views)
    tile = jnp.floor(high * (1.0 / ratio))
    low_row = as_row(low + DIGIT * (high - ratio * tile), capacity)
    wanted = lax.broadcasted_iota(jnp.int32, (TILE, lanes), 0).astype(jnp.float32)
    for at in range(0, entries, lanes):
        same = (wanted == low_row[:, at : at + lanes]).astype(jnp.float32)
        same_ref[:, at : at + lanes] = same.astype(jnp.bfloat16)
    tile_column = as_column(tile, capacity)
    tile_ref[...] = tile_column.astype(jnp.bfloat16)
    lane = lax.broadcasted_iota(jnp.int32, (entries, lanes), 1).astype(jnp.float32)
    in_tile = (tile_column == lane).astype(jnp.float32).astype(jnp.bfloat16)
    number_ref[...] = jnp.dot(same_ref[...], in_tile, preferred_element_type=jnp.float32)


def dense_prepare_kernel(*refs):
    *in_refs, same_ref, tile_ref, number_ref = refs
    prepare_tiles(own_bucket(in_refs), same_ref, tile_ref, number_ref)


def dense_prepare(parts):
    pairs, rows, lanes = parts[0].shape
    entries = len(parts) * pairs * (rows - META) // 2
    return pl.pallas_call(
        dense_prepare_kernel,
        out_shape=[
            jax.ShapeDtypeStruct((TILE, entries), jnp.bfloat16),
            jax.ShapeDtypeStruct((entries, lanes), jnp.bfloat16),
            jax.ShapeDtypeStruct((TILE, lanes), jnp.float32),
        ],
        in_specs=[vmem_spec()] * len(parts),
        out_specs=[vmem_spec()] * 3,
        compiler_params=grant(8 * MIB),
        name="dense_prepare",
    )(*parts)


def pair_sums(pair, views, same_refs, tile_refs):
    values = entries_of(views)
    tile_of = jnp.concatenate([ref[...] for ref in tile_refs], axis=0)
    same = jnp.concatenate([ref[...] for ref in same_refs], axis=1)
    zero = jnp.zeros_like(values)
    picked = jnp.concatenate([jnp.where(tile_of == 2 * pair + k, values, zero) for k in range(2)], axis=1)
    return jnp.dot(same, picked, preferred_element_type=jnp.float32)


def begin_tiles_kernel(*refs):
    *in_refs, same_ref, tile_ref, out_ref = refs
    views = own_bucket(in_refs)
    lanes = out_ref.shape[1]
    for pair in range(BUCKET // (2 * TILE)):
        sums = pair_sums(pair, views, [same_ref], [tile_ref])
        for k in range(2):
            out_ref[pl.ds((2 * pair + k) * TILE, TILE), :] = sums[:, k * lanes : (k + 1) * lanes]


def begin_tiles(parts, prepared):
    lanes = parts[0].shape[2]
    return pl.pallas_call(
        begin_tiles_kernel,
        out_shape=jax.ShapeDtypeStruct((BUCKET, lanes), jnp.float32),
        in_specs=[vmem_spec()] * (len(parts) + 2),
        out_specs=vmem_spec(),
        compiler_params=grant(8 * MIB),
        name="begin_tiles",
    )(*parts, *prepared[:2])


def finish_tiles_kernel(count, *refs):
    same_parts, other_parts = refs[:count], refs[count : 2 * count]
    begun_ref, number_ref, *middle = refs[2 * count : 2 * count + 5]
    out_ref, mean_ref, inverse_ref, same_ref, tile_ref, last_ref, sems = refs[2 * count + 5 :]
    prepare_tiles(own_bucket(other_parts), same_ref, tile_ref, last_ref)
    views = own_bucket(same_parts + other_parts)
    lanes = mean_ref.shape[1]
    inverse_ref[...] = 1.0 / jnp.maximum(number_ref[...] + middle[2][...] + last_ref[...], 1.0)
    copies = []
    for pair in range(sems.shape[0]):
        sums = pair_sums(pair, views, [middle[0], same_ref], [middle[1], tile_ref])
        for k in range(2):
            tile = 2 * pair + k
            where = pl.ds(tile * TILE, TILE)
            total = begun_ref[where, :] + sums[:, k * lanes : (k + 1) * lanes]
            mean_ref[where, :] = total * inverse_ref[:, tile : tile + 1]
            copy = pltpu.make_async_copy(mean_ref.at[where], out_ref.at[where], sems.at[pair, k])
            copy.start()
            copies.append(copy)
    for copy in copies:
        copy.wait()


def finish_tiles(same_parts, other_parts, begun, number, middle):
    pairs, rows, lanes = other_parts[0].shape
    entries = len(other_parts) * pairs * (rows - META) // 2
    return pl.pallas_call(
        functools.partial(finish_tiles_kernel, len(other_parts)),
        out_shape=jax.ShapeDtypeStruct((BUCKET, lanes), jnp.float32),
        in_specs=[vmem_spec()] * (2 * len(other_parts) + 5),
        out_specs=hbm_spec(),
        scratch_shapes=[
            pltpu.VMEM((BUCKET, lanes), jnp.float32),
            pltpu.VMEM((TILE, lanes), jnp.float32),
            pltpu.VMEM((TILE, entries), jnp.bfloat16),
            pltpu.VMEM((entries, lanes), jnp.bfloat16),
            pltpu.VMEM((TILE, lanes), jnp.float32),
            pltpu.SemaphoreType.DMA((BUCKET // (2 * TILE), 2)),
        ],
        cost_estimate=dense_cost(entries, lanes, 2.0),
        compiler_params=pltpu.CompilerParams(vmem_limit_bytes=16 * MIB),
        name="finish_tiles",
    )(*same_parts, *other_parts, begun, number, *middle)


def by_pairs(values, slots, counts, groups):
    members = values.shape[0]
    pairs = members // 2

    def swap(array, axis, size, by):
        return lax.ppermute(array, axis, [(i, i ^ by) for i in range(size)])

    sent = pack(values, slots, counts, groups, True)
    mine = [sent[0]] + [swap(sent[k], "mem", members, 2 * k) for k in range(1, pairs)]
    mine = jnp.stack(mine, axis=0)
    same = [mine] + [swap(mine, "grp", groups, k) for k in range(1, groups)]
    other = [swap(part, "mem", members, 1) for part in same]
    first = [same[0], other[0]]
    begun = begin_answer(first)
    early = dense_prepare(first)
    sums = begin_tiles(first, early)
    begun = more_answer(same[1:], begun)
    prepared = dense_prepare(same[1:])
    begun = more_answer(other[2:], begun)
    answers = finish_answer(other[1:2], begun)
    averaged = finish_tiles(same[1:], other[1:], sums, early[2], prepared)
    back = [answers[0]] + [swap(answers[k], "mem", members, 2 * k) for k in range(1, pairs)]
    return averaged, place(back)


def by_all(values, slots, counts, groups):
    members = values.shape[0]
    (lists,) = pack(values, slots, counts, groups, False)
    got = lax.all_to_all(lists, ("grp", "mem"), split_axis=0, concat_axis=0, tiled=True)
    back = answer(got, members)
    returned = lax.all_to_all(back, "mem", split_axis=0, concat_axis=0, tiled=True)
    return dense(got), returned


def per_device(groups, values, slots, counts):
    members, capacity, lanes = values.shape[1:]
    entries = groups * members * capacity
    few = members == 8 and groups in (4, 8) and entries <= 2048 and 4 * capacity == lanes
    tiles = BUCKET % (2 * TILE) == 0 and BUCKET // TILE <= lanes
    move = by_pairs if few and tiles else by_all
    averaged, returned = move(values[0], slots[0], counts, groups)
    return (averaged, returned[None])


def one_step(groups, values, slots, counts):
    return per_device(groups, values, slots, counts)


def solution(mesh):
    return jax.shard_map(
        functools.partial(one_step, mesh.shape["grp"]),
        mesh=mesh,
        in_specs=(
            P(("grp", "mem"), None, None, None),
            P(("grp", "mem"), None, None),
            P(("grp", "mem"), None),
        ),
        out_specs=(P("mem", None), P(("grp", "mem"), None, None, None)),
        check_vma=False,
    )
```
